128 devices in a mesh: rep: 2 (over core), dp: 64 (over x, y, z).
Axes of the slice: x: 4, y: 4, z: 4, core: 2. Of those that a mesh axis runs over, the one named last changes fastest.
Arguments:
- g_w_gate: bfloat16 [128, 2, 768, 1792], P(('rep', 'dp')), parts along dimension 0
- g_w_up: bfloat16 [128, 2, 768, 1792], P(('rep', 'dp')), parts along dimension 0
- g_w_down: bfloat16 [128, 2, 1792, 768], P(('rep', 'dp')), parts along dimension 0
- w_gate: bfloat16 [2, 768, 1792], replicated
- w_up: bfloat16 [2, 768, 1792], replicated
- w_down: bfloat16 [2, 1792, 768], replicated
- m_w_gate: float32 [2, 768, 1792], P(None, 'dp')
- m_w_up: float32 [2, 768, 1792], P(None, 'dp')
- m_w_down: float32 [2, 1792, 768], P(None, 'dp')
- v_w_gate: float32 [2, 768, 1792], P(None, 'dp')
- v_w_up: float32 [2, 768, 1792], P(None, 'dp')
- v_w_down: float32 [2, 1792, 768], P(None, 'dp')
Outputs:
- output 1: bfloat16 [4, 768, 1792], P('rep'), parts along dimension 0
- output 2: bfloat16 [4, 768, 1792], P('rep'), parts along dimension 0
- output 3: bfloat16 [4, 1792, 768], P('rep'), parts along dimension 0
- output 4: float32 [4, 768, 1792], P('rep', 'dp'), parts along dimension 0
- output 5: float32 [4, 768, 1792], P('rep', 'dp'), parts along dimension 0
- output 6: float32 [4, 1792, 768], P('rep', 'dp'), parts along dimension 0
- output 7: float32 [4, 768, 1792], P('rep', 'dp'), parts along dimension 0
- output 8: float32 [4, 768, 1792], P('rep', 'dp'), parts along dimension 0
- output 9: float32 [4, 1792, 768], P('rep', 'dp'), parts along dimension 0
There are 2 independent parts. The reference program is written for one: setup_inputs(seed, part) draws one part's arguments, and reference() takes and returns one part's arrays. A program takes and returns all parts, laid end to end along the dimension named above; an argument that names none is the same for every part.
All inputs are finite; a program needn't handle non-finite values.
Results may differ from the reference program's by a relative error of at most 0.022.
Values are sent between devices in bfloat16 or wider.
A program may use at most 1.5 GiB of HBM per device.

```python
import jax
import jax.numpy as jnp
from jax import lax

DEVICES = 64
D = 768
FF = 1792
LAYERS = 2
NAMES = ("w_gate", "w_up", "w_down")
SHAPES = {"w_gate": (LAYERS, D, FF), "w_up": (LAYERS, D, FF), "w_down": (LAYERS, FF, D)}


def setup_inputs(seed: int = 0, part: int = 0) -> dict:
    kz, *keys = jax.random.split(jax.random.key(seed), 1 + 5 * len(NAMES))
    loud = 2.0 ** jax.random.uniform(kz, (), jnp.float32, -1.0, 1.0)
    drawn = {}
    for name, key, both in zip(NAMES, keys[:3], keys[3:6], strict=True):
        own = jax.random.normal(jax.random.fold_in(key, part), (DEVICES, *SHAPES[name]), jnp.float32)
        shared = jax.random.normal(jax.random.fold_in(both, part), SHAPES[name], jnp.float32)
        drawn["g_" + name] = (loud * (0.7 * shared / DEVICES + 0.7 * own * DEVICES**-0.5)).astype(jnp.bfloat16)
    for name, key in zip(NAMES, keys[6:9], strict=True):
        drawn[name] = (jax.random.normal(key, SHAPES[name], jnp.float32) * SHAPES[name][1] ** -0.5).astype(jnp.bfloat16)
    for name, key in zip(NAMES, keys[9:12], strict=True):
        drawn["m_" + name] = loud * 0.5 * jax.random.normal(key, SHAPES[name], jnp.float32)
    for name, key in zip(NAMES, keys[12:15], strict=True):
        drawn["v_" + name] = loud * loud * jax.random.uniform(key, SHAPES[name], jnp.float32, 0.5, 1.5)
    return drawn


def adamw(w, m, v, g):
    m = 0.9 * m + 0.1 * g
    v = 0.95 * v + 0.05 * g * g
    step = m * lax.rsqrt(v + 1e-8) + 0.1 * w
    return (w - 0.02 * step).astype(jnp.bfloat16), m, v


def clipped(gradients, sum_of_squares, count):
    factor = jnp.minimum(1.0, 0.5 * lax.rsqrt(sum_of_squares / count + 1e-30))
    return [g * factor for g in gradients]


def reference(g_w_gate, g_w_up, g_w_down, w_gate, w_up, w_down, m_w_gate, m_w_up, m_w_down, v_w_gate, v_w_up, v_w_down):
    def total(terms):
        return lax.scan(lambda so_far, term: (so_far + term.astype(jnp.float32), None), jnp.zeros(terms.shape[1:], jnp.float32), terms)[0]

    gradients = [total(terms).astype(jnp.bfloat16).astype(jnp.float32) for terms in (g_w_gate, g_w_up, g_w_down)]
    gradients = clipped(gradients, sum(jnp.sum(g * g) for g in gradients), sum(g.size for g in gradients))
    new = [
        adamw(w.astype(jnp.float32), m, v, g)
        for w, m, v, g in zip((w_gate, w_up, w_down), (m_w_gate, m_w_up, m_w_down), (v_w_gate, v_w_up, v_w_down), gradients, strict=True)
    ]
    return tuple(one[which] for which in range(3) for one in new)
```

```python
import jax
import jax.numpy as jnp
from jax import lax
from jax.experimental import pallas as pl
from jax.experimental.pallas import tpu as pltpu
from jax.sharding import PartitionSpec as P

UP, DOWN, GATE = WEIGHTS = range(3)
N = 4
QUARTERS = range(N)
FLOWS = BOTH = range(2)
ALL = [(w, h) for h in FLOWS for w in WEIGHTS]
STRIDE = {"x": N * N, "y": N, "z": 1}
AXES = (("x", "y", "z"), ("y", "z", "x"), ("z", "x", "y"))
CHUNK_AXIS = ("y", "x", "x")
FAR_FIRST = (2, 1, 3)
OUTWARD = (0, -1, 1, 2)
NEAR = (-1, 1)
TILE = 16
BF, F32 = jnp.bfloat16, jnp.float32


def fori(n, body):
    lax.fori_loop(0, n, lambda i, c: (body(i), c)[1], 0)


def main_kernel(names, count, *refs):
    R = dict(zip(names, refs, strict=True))

    def three(name):
        return [R[name, w] for w in WEIGHTS]

    g, wt, mi, vi, W, mo, vo = (three(n) for n in ("g", "wt", "mi", "vi", "W", "mo", "vo"))
    own1, own2, r, ws, ms, vs, pieces = (three(n) for n in ("own1", "own2", "r", "ws", "ms", "vs", "pieces"))
    wl, mv = ([R[n, UP], R[n, DOWN], R[n, UP]] for n in ("wl", "mv"))
    tall = [R["tall", UP], R["tall", DOWN], R["tall", UP]]
    qa = {w: R["qa", w] for w in (UP, GATE)}
    gf = mo
    pb, bs, qb, bt, rb, fa, sa, ra, fc, sc, rc, tsc, tc, ub, uc, vc, nsend, nrecv = (
        R[n] for n in ("pb", "bs", "qb", "bt", "rb", "fa", "sa", "ra", "fc", "sc", "rc", "tsc", "tc", "ub", "uc", "vc", "nsend", "nrecv")
    )
    ua = sa
    sent, local, rec1, rec2, rec2b, rec3, recn, rech, recy, reco = (
        R[n] for n in ("sent", "local", "rec1", "rec2", "rec2b", "rec3", "recn", "rech", "recy", "reco")
    )
    tokens = iter(range(sent.shape[0]))
    leaving = []

    me = lax.axis_index("dp")
    co = {"x": me // STRIDE["x"], "y": me // STRIDE["y"] % N, "z": me % N}
    x, y, z = co["x"], co["y"], co["z"]

    def at(axis, off):
        return (co[axis] + off) % N

    def to(axis, off):
        return me + (at(axis, off) - co[axis]) * STRIDE[axis]

    def group(ref):
        sem = sent.at[next(tokens)]
        leaving.append((ref, sem))
        return sem

    def post(src, dst, ssem, rsem, device):
        pltpu.make_async_remote_copy(
            src_ref=src, dst_ref=dst, send_sem=ssem, recv_sem=rsem, device_id={"dp": device}, device_id_type=pl.DeviceIdType.MESH
        ).start()

    def send(src, dst, ssem, rsem, axis, off):
        post(src, dst, ssem, rsem, to(axis, off))

    def wait(ref, sem):
        pltpu.make_async_copy(ref, ref, sem).wait()

    def way(h):
        return 1 - 2 * h

    def offs(w, h):
        return (2, 1, -1, 0) if w == DOWN else (2, -way(h), way(h), 0)

    def term(w, h, q, c):
        if w == UP:
            return g[w].at[h, q, c]
        if w == DOWN:
            return g[w].at[h, c, q]
        cols = g[w].shape[-1] // 2
        return g[w].at[q // 2, c, h, :, pl.ds(pl.multiple_of(q % 2 * cols, 128), cols)]

    def tiles(n, body):
        fori(n // TILE, lambda i: body(pl.ds(pl.multiple_of(i * TILE, TILE), TILE)))

    def cut(w):
        rows, (_, pad, cols) = vi[w].shape[0], pieces[w].shape
        for q in QUARTERS:
            pieces[w][q] = tall[w][rows * q : rows * q + pad, 0:cols]

    def join(w, piece, cols):
        rows = vi[w].shape[0]
        for q in QUARTERS:
            tall[w][rows * q : rows * q + rows, 0:cols] = piece(q).astype(F32)[:rows]
        return tall[w][0 : N * rows, 0:cols].astype(BF)

    barrier = pltpu.get_barrier_semaphore()
    for axis in STRIDE:
        for off in FAR_FIRST:
            pl.semaphore_signal(barrier, inc=1, device_id={"dp": to(axis, off)}, device_id_type=pl.DeviceIdType.MESH)

    for which, buf in enumerate((own1, own2)):
        for w, h in ALL:
            q = at(AXES[w][0], way(h) * (1 - which))
            for k in QUARTERS:
                src = term(w, h, q, at(CHUNK_AXIS[w], offs(w, h)[k]))
                pltpu.make_async_copy(src, buf[w].at[h, k], local.at[which, w, h]).start()
    pl.semaphore_wait(barrier, len(STRIDE) * len(FAR_FIRST))

    left1 = [group(r[w]) for w in WEIGHTS]

    def phase1(i, w, h, k, src, off):
        send(src, r[w].at[i, h, k], left1[w], rec1.at[w, i, h, k], AXES[w][0], off)

    for i, (far, near) in enumerate(((2, 1), (-1, -1))):
        for k in QUARTERS:
            for w, h in ALL:
                s = way(h)
                src = term(w, h, at(AXES[w][0], far * s), at(CHUNK_AXIS[w], offs(w, h)[k]))
                phase1(i, w, h, k, src, near * s)

    def load_state(w):
        for i, (src, dst) in enumerate(((wt[w].at[:, x, y], wl[w]), (mi[w], mv[w].at[0]), (vi[w], mv[w].at[1]))):
            pltpu.make_async_copy(src, dst, local.at[2 + i // 2, w, i % 2]).start()

    load_state(UP)
    load_state(DOWN)
    for which, buf in enumerate((own1, own2)):
        for w, h in ALL:
            wait(buf[w].at[h], local.at[which, w, h])

    for k in QUARTERS:
        for w, h in ALL:
            wait(r[w].at[0, h, k], rec1.at[w, 0, h, k])

            def add(t, w=w, h=h, k=k):
                own1[w][h, k, t] = (own1[w][h, k, t].astype(F32) + r[w][0, h, k, t].astype(F32)).astype(BF)

            tiles(own1[w].shape[2], add)
            phase1(2, w, h, k, own1[w].at[h, k], way(h))

    for w in WEIGHTS:
        rows, (_, pad, cols) = vi[w].shape[0], ms[w].shape
        if w != GATE:
            n = N * rows
            tall[w][n : n + TILE, :] = jnp.zeros((TILE, tall[w].shape[1]), F32)
        for i, dst in enumerate((wl[w], mv[w].at[0], mv[w].at[1])):
            wait(dst, local.at[2 + i // 2, w, i % 2])
        for h in BOTH:
            for dst in (ms[w], vs[w]):
                dst[h, pad - 8 : pad] = jnp.zeros((8, cols), F32)

        def spread(i, w=w):
            for src, dst in ((mv[w][0, i], ms[w]), (mv[w][1, i], vs[w])):
                for h in BOTH:
                    dst[h, pl.ds(i, 1), :] = src[h : h + 1]

        fori(rows, spread)
        for h in BOTH:

            def widen(t, w=w, h=h):
                tall[w][t, :] = wl[w][h, t].astype(F32)

            tiles(N * rows, widen)
            src = pieces[w] if w != GATE else pieces[UP]
            cut(w if w != GATE else UP)
            ws[w][h] = src[z]
        if w == UP:
            load_state(GATE)

    def total(w, h, k, t):
        return own2[w][h, k, t].astype(F32) + r[w][1, h, k, t].astype(F32) + r[w][2, h, k, t].astype(F32)

    def cut_down(h, k):
        def put(t):
            tall[DOWN][t, :] = total(DOWN, h, k, t)

        tiles(own2[DOWN].shape[2], put)
        cut(DOWN)

    left2 = {w: group(qa[w]) for w in qa}
    left2b = group(qb)

    def phase2(i, w, h, off):
        send(own2[w].at[h, i], qa[w].at[h, i], left2[w], rec2.at[w // 2, h, i], AXES[w][1], off)

    def phase2b(i, h, k, off):
        send(bs.at[h, k, i], qb.at[h, k, i], left2b, rec2b.at[h, k, i], "z", off)

    for k in QUARTERS:
        for w, h in ALL:
            s = way(h)
            for i in (1, 2):
                wait(r[w].at[i, h, k], rec1.at[w, i, h, k])
            if w == DOWN:
                cut_down(h, k)
                pb[h, k] = pieces[w][z]
                for i, (far, near) in enumerate(((2, 1), (-1, -1))):
                    bs[h, k, i] = pieces[w][at("z", far * s)].astype(BF)
                    phase2b(i, h, k, near * s)
            elif k < 2:

                def put(t, w=w, h=h, k=k):
                    own2[w][h, k, t] = total(w, h, k, t).astype(BF)

                tiles(own2[w].shape[2], put)
                phase2(k, w, h, -s if k else s)

    for w, h in ALL:
        s = way(h)
        if w == DOWN:
            for k in QUARTERS:
                cut_down(h, k)
                wait(qb.at[h, k, 0], rec2b.at[h, k, 0])
                bs[h, k, 2] = (pieces[w][at("z", s)] + qb[h, k, 0].astype(F32)).astype(BF)
                phase2b(2, h, k, s)
        else:
            wait(qa[w].at[h, 0], rec2.at[w // 2, h, 0])

            def add2(t, w=w, h=h):
                own2[w][h, 2, t] = (total(w, h, 2, t) + qa[w][h, 0, t].astype(F32)).astype(BF)

            tiles(own2[w].shape[2], add2)
            phase2(2, w, h, s)

    left_a, left_c, left_b = group(ra), group(rc), group(rb)
    for w in qa:
        for h in BOTH:
            for i in (1, 2):
                wait(qa[w].at[h, i], rec2.at[w // 2, h, i])

            def total2(t, w=w, h=h):
                return total(w, h, 3, t) + qa[w][h, 1, t].astype(F32) + qa[w][h, 2, t].astype(F32)

            if w == UP:

                def put2(t, total2=total2):
                    tall[UP][t, :] = total2(t)

                tiles(own2[w].shape[2], put2)
                cut(UP)
                for q in QUARTERS:
                    sa[q, h] = pieces[UP][q].astype(BF)
                fa[h] = pieces[UP][z]
            else:
                n = fc.shape[1]
                for b in BOTH:

                    def put2(i, total2=total2, h=h, b=b, n=n):
                        v = total2(pl.ds(pl.multiple_of(b * n + i * TILE, TILE), TILE))
                        t = pl.ds(pl.multiple_of(i * TILE, TILE), TILE)
                        fc[2 * h + b, t] = v
                        sc[2 * h + b, t] = v.astype(BF)

                    fori(n // TILE, put2)
        for j in FAR_FIRST:
            if w == UP:
                send(sa.at[at("z", j)], ra.at[j - 1], left_a, rec3.at[0, j - 1], "z", j)
            else:
                send(sc.at[at("y", j)], rc.at[j - 1], left_c, rec3.at[1, j - 1], "y", j)
    for k in QUARTERS:
        for h in BOTH:
            for i in (1, 2):
                wait(qb.at[h, k, i], rec2b.at[h, k, i])
            v = pb[h, k] + qb[h, k, 1].astype(F32) + qb[h, k, 2].astype(F32)
            off = offs(DOWN, h)[k]
            if off:
                bt[h, k] = v.astype(BF)
                send(bt.at[h, k], rb.at[h, k], left_b, rec3.at[2 + h, k], "x", off)
            else:
                pb[h, k] = v

    def fold(v):
        v = jnp.sum(v * v, axis=0, keepdims=True)
        out = v[:, 0:128]
        for i in range(128, v.shape[1], 128):
            out = out + v[:, i : i + 128]
        nsend[...] = nsend[...] + out

    def valid(n, v):
        return jnp.where(lax.broadcasted_iota(jnp.int32, v.shape, 0) < n, v, 0.0)

    def rounded(own, others):
        for o in others:
            own = own + o.astype(F32)
        return own.astype(BF).astype(F32)

    others = range(len(FAR_FIRST))
    half = tsc.shape[-1]
    nsend[...] = jnp.zeros(nsend.shape, F32)
    for j in others:
        wait(rc.at[j], rec3.at[1, j])

    def last_c(t):
        v = rounded(fc[y, t], [rc[j, t] for j in others])
        tall[UP][t, 0:half] = v
        fold(v)

    tiles(fc.shape[1], last_c)
    cut(GATE)
    for q in QUARTERS:
        tsc[q] = pieces[GATE][q].astype(BF)
    tc[z] = tsc[z]
    left = group(tc.at[0:3])
    for j in FAR_FIRST:
        send(tsc.at[at("z", j)], tc.at[z], left, rech.at[0, j - 1], "z", j)
    for j in others:
        wait(ra.at[j], rec3.at[0, j])
    (gone,) = [i for i, (_, sem) in enumerate(leaving) if sem is left_a]
    wait(*leaving.pop(gone))
    for h in BOTH:
        v = rounded(fa[h], [ra[j, h] for j in others])
        gf[UP][h] = v
        fold(valid(vi[UP].shape[0], v))
    for h in BOTH:
        for k in others:
            wait(rb.at[h, k], rec3.at[2 + h, k])
        v = rounded(pb[h, 3], [rb[h, k] for k in others])
        gf[DOWN][h] = v
        fold(valid(vi[DOWN].shape[0], v))

    devices = nrecv.shape[0]
    nrecv[me] = nsend[...]
    left = group(nrecv.at[1:devices])
    fori(devices - 1, lambda i: post(nsend, nrecv.at[me], left, recn.at[0], (me + 1 + i) % devices))
    for j in FAR_FIRST:
        wait(tc.at[at("z", -j)], rech.at[0, j - 1])
    wait(nrecv.at[1:devices], recn.at[0])
    squares = jnp.sum(jnp.sum(nrecv[...], axis=0), axis=1, keepdims=True)
    factor = jnp.minimum(1.0, 0.5 * lax.rsqrt(squares / count + 1e-30))
    for q in QUARTERS:
        gf[GATE][q // 2, :, half * (q % 2) : half * (q % 2 + 1)] = tc[q].astype(F32)

    def adamw(w, h):
        gc = gf[w][h] * factor
        m = 0.9 * ms[w][h] + 0.1 * gc
        v = 0.95 * vs[w][h] + 0.05 * gc * gc
        mo[w][h] = m
        vo[w][h] = v
        step = m * lax.rsqrt(v + 1e-8) + 0.1 * ws[w][h]
        return (ws[w][h] - 0.02 * step).astype(BF)

    def spread_out(i, axis, ref, src, first):
        left = group(first)
        for j in FAR_FIRST:
            send(src(at(axis, j)), ref(co[axis]), left, rech.at[i, j - 1], axis, j)

    def arrived(i, axis, ref):
        for j in FAR_FIRST:
            wait(ref(at(axis, -j)), rech.at[i, j - 1])

    for h in BOTH:
        new = adamw(GATE, h)
        vc[2 * h] = new[:, :half]
        vc[2 * h + 1] = new[:, half:]
    uc[z] = vc[z]
    spread_out(1, "z", lambda p: uc.at[p], lambda p: vc.at[p], uc.at[0:3])
    for h in BOTH:
        ua[z, h] = adamw(UP, h)
    spread_out(2, "z", lambda p: ua.at[p], lambda p: ua.at[z], ua.at[0:3])
    for h in BOTH:
        ub[z, x, h] = adamw(DOWN, h)
    spread_out(3, "x", lambda p: ub.at[z, p], lambda p: ub.at[z, x], ub.at[0, 0:3])

    def own_out(block, left, recv, axis):
        for d in BOTH:
            ref = block(0, None)
            send(ref, ref, left, recv.at[0, d], axis, way(d))

    def pass_on(block, left, recv, axis):
        for d in BOTH:
            wait(block(NEAR[d], None), recv.at[0, d])
            ref = block(NEAR[d], d)
            send(ref, ref, left, recv.at[1, d], axis, way(d))

    def passed(block, recv):
        for d in BOTH:
            wait(block(2, d), recv.at[1, d])

    def ring(ref, sub):
        def block(p, d):
            one = ref(p)
            return one if d is None else one.at[sub(d)]

        return block

    def one(d):
        return d

    def two(d):
        return pl.ds(2 * d, 2)

    left_o = [group(W[w].at[0:3]) for w in WEIGHTS]

    def outer(w, i):
        return ring(lambda p: W[w].at[at(AXES[w][0], p), at(CHUNK_AXIS[w], OUTWARD[i])], two if w == GATE else one)

    def outer_start(w, i):
        own_out(outer(w, i), left_o[w], reco.at[w, i], AXES[w][0])

    left_z, left_y, left_x = group(ub.at[0:3]), group(W[UP].at[0, 0:3]), group(W[GATE].at[0, 0:3])
    zring = [ring(lambda p, off=off: ub.at[at("z", p), at("x", off)], one) for off in OUTWARD]
    own_out(zring[0], left_z, recy.at[2], "z")

    arrived(1, "z", lambda p: uc.at[p])
    W[GATE][z, x, y] = join(GATE, lambda q: uc[q], half)
    spread_out(4, "y", lambda p: W[GATE].at[z, x, p], lambda p: W[GATE].at[z, x, y], W[GATE].at[0, 0, 0:3])

    arrived(2, "z", lambda p: ua.at[p])
    for h in BOTH:
        W[UP][x, y, h] = join(UP, lambda q: ua[q, h], tall[UP].shape[1])
    yring = ring(lambda p: W[UP].at[x, at("y", p)], one)
    own_out(yring, left_y, recy.at[0], "y")
    outer_start(UP, 0)

    for i, off in enumerate(OUTWARD):
        if off:
            wait(ub.at[z, at("x", off)], rech.at[3, -off % N - 1])
            own_out(zring[i], left_z, recy.at[2 + i], "z")
    for i in QUARTERS:
        pass_on(zring[i], left_z, recy.at[2 + i], "z")

    arrived(4, "y", lambda p: W[GATE].at[z, x, p])
    xring = ring(lambda p: W[GATE].at[z, at("x", p)], two)
    own_out(xring, left_x, recy.at[1], "x")
    outer_start(GATE, 0)

    pass_on(yring, left_y, recy.at[0], "y")
    outer_start(UP, 1)
    outer_start(UP, 2)
    for i in QUARTERS:
        passed(zring[i], recy.at[2 + i])
        c = at("x", OUTWARD[i])
        for h in BOTH:
            W[DOWN][y, c, h] = join(DOWN, lambda q: ub[q, c, h], tall[DOWN].shape[1])
        outer_start(DOWN, i)
    pass_on(xring, left_x, recy.at[1], "x")
    outer_start(GATE, 1)
    outer_start(GATE, 2)
    passed(yring, recy.at[0])
    outer_start(UP, 3)
    passed(xring, recy.at[1])
    outer_start(GATE, 3)
    for i in QUARTERS:
        for w in WEIGHTS:
            pass_on(outer(w, i), left_o[w], reco.at[w, i], AXES[w][0])
    for i in QUARTERS:
        for w in WEIGHTS:
            passed(outer(w, i), reco.at[w, i])
    for ref, sem in leaving:
        wait(ref, sem)


def write_kernel(names, *refs):
    R = dict(zip(names, refs, strict=True))
    W = [R["W", w] for w in WEIGHTS]
    out = [R["out", w] for w in WEIGHTS]
    half = W[GATE].shape[-1]
    copies = []
    for p in QUARTERS:
        for h in BOTH:
            cols, two = pl.ds(half * (p % 2), half), pl.ds(2 * h, 2)
            pairs = (
                (W[UP].at[p, :, h], out[UP].at[h, p]),
                (W[DOWN].at[p, :, h], out[DOWN].at[h, :, p]),
                (W[GATE].at[p, two], out[GATE].at[p // 2, two, :, :, cols]),
            )
            copies += [pltpu.make_async_copy(*pair, R["sem"].at[w, p, h]) for w, pair in enumerate(pairs)]
    for c in copies:
        c.start()
    for w in WEIGHTS:

        def gather(i, w=w):
            for n in "mv":
                for h in BOTH:
                    R[n + "b", w][i, h : h + 1] = R[n + "o", w][h, pl.ds(i, 1), :]

        fori(R["mb", w].shape[0], gather)
        for i, n in enumerate("mv"):
            copies.append(pltpu.make_async_copy(R[n + "b", w], R[n + "out", w], R["small"].at[i, w]))
            copies[-1].start()
    for c in copies:
        c.wait()


def call(kernel, ins, outs, scratch, place_in, place_out, **params):
    names = (*ins, *outs, *scratch)
    got = pl.pallas_call(
        lambda *refs: kernel(names, *refs),
        out_shape=list(outs.values()),
        in_specs=[pl.BlockSpec(memory_space=place_in)] * len(ins),
        out_specs=[pl.BlockSpec(memory_space=place_out)] * len(outs),
        scratch_shapes=list(scratch.values()),
        name=kernel.__name__,
        compiler_params=pltpu.CompilerParams(**params),
    )(*ins.values())
    return dict(zip(outs, got, strict=True))


def by_weight(**of):
    return {(n, w): t for n, ts in of.items() for w, t in zip(WEIGHTS, ts)}


def solution(mesh):
    def step(*arrays):
        terms, weights, m, v = ([arrays[i + j] for j in (1, 2, 0)] for i in (0, 3, 6, 9))
        (rows, ff), (rows_d, d) = m[0].shape[1:], m[1].shape[1:]
        half, n, n_d = ff // 2, N * rows, N * rows_d
        full = ((2, N, N, n, ff), (2, N, N, n_d, d), (2, N, N, n, ff))
        g = [t.reshape(s) for t, s in zip(terms, (*full[:2], (2, N, 2, 2 * n, ff)))]
        state = [[pltpu.with_memory_space_constraint(a.transpose(1, 0, 2), pltpu.HBM) for a in t] for t in (m, v)]
        weights = [a.reshape(s) for a, s in zip(weights, full)]
        ins = by_weight(g=g, wt=weights, mi=state[0], vi=state[1])

        vm, dma = pltpu.VMEM, pltpu.SemaphoreType.DMA
        pad, pad_d = 16, 32
        chunk = ((n, ff), (n_d, d), (2 * n, half))
        own = ((2, pad, ff), (2, pad_d, d), (2, pad, ff))
        pieces = [vm((N, *s), F32) for s in ((pad, ff), (pad_d, d), (pad, half))]
        scratch = by_weight(
            own1=[vm((2, N, *c), BF) for c in chunk],
            own2=[vm((2, N, *c), BF) for c in chunk],
            r=[vm((3, 2, N, *c), BF) for c in chunk],
            ws=[vm(s, F32) for s in own],
            ms=[vm(s, F32) for s in own],
            vs=[vm(s, F32) for s in own],
            pieces=pieces,
            wl=[vm((2, *c), BF) for c in chunk[:2]],
            mv=[vm((2, *a.shape), F32) for a in state[0][:2]],
            tall=[vm((n + TILE, ff), F32), vm((n_d + TILE, d), F32)],
        )
        scratch |= {("qa", w): vm((2, 3, *chunk[w]), BF) for w in (UP, GATE)}
        scratch |= dict(
            pb=vm((2, N, pad_d, d), F32),
            bs=vm((2, N, 3, pad_d, d), BF),
            qb=vm((2, N, 3, pad_d, d), BF),
            bt=vm((2, 3, pad_d, d), BF),
            rb=vm((2, 3, pad_d, d), BF),
            fa=vm((2, pad, ff), F32),
            sa=vm((N, 2, pad, ff), BF),
            ra=vm((3, 2, pad, ff), BF),
            fc=vm((N, n, half), F32),
            sc=vm((N, n, half), BF),
            rc=vm((3, n, half), BF),
            tsc=vm((N, pad, half), BF),
            tc=vm((N, pad, half), BF),
            ub=vm((N, N, 2, pad_d, d), BF),
            uc=vm((N, pad, half), BF),
            vc=vm((N, pad, half), BF),
            nsend=vm((1, 128), F32),
            nrecv=vm((N**3, 1, 128), F32),
            sent=dma((24,)),
            local=dma((N, 3, 2)),
            rec1=dma((3, 3, 2, N)),
            rec2=dma((2, 2, 3)),
            rec2b=dma((2, N, 3)),
            rec3=dma((N, 3)),
            recn=dma((1,)),
            rech=dma((5, 3)),
            recy=dma((6, 2, 2)),
            reco=dma((3, N, 2, 2)),
        )
        outs = by_weight(
            W=[jax.ShapeDtypeStruct(s, BF) for s in ((N, N, 2, n, ff), (N, N, 2, n_d, d), (N, N, N, n, half))],
            mo=[jax.ShapeDtypeStruct(s, F32) for s in own],
            vo=[jax.ShapeDtypeStruct(s, F32) for s in own],
        )
        count = float(N**3 * sum(a.size for a in m))

        def main(names, *refs):
            main_kernel(names, count, *refs)

        got = call(main, ins, outs, scratch, pltpu.HBM, vm, collective_id=0, has_side_effects=True, vmem_limit_bytes=36900000)
        small = [jax.ShapeDtypeStruct(a.shape, F32) for a in state[0]]
        outs = by_weight(out=[jax.ShapeDtypeStruct(s, BF) for s in full], mout=small, vout=small)
        scratch = by_weight(mb=[vm(a.shape, F32) for a in small], vb=[vm(a.shape, F32) for a in small])
        scratch |= dict(sem=dma((3, N, 2)), small=dma((2, 3)))
        new = call(write_kernel, got, outs, scratch, vm, pltpu.HBM, vmem_limit_bytes=2000000)
        back = (GATE, UP, DOWN)
        whole = [new["out", w].reshape(2, -1, full[w][-1]) for w in back]
        return (*whole, *(new[n, w].transpose(1, 0, 2) for n in ("mout", "vout") for w in back))

    all_of, part = P(None, None, None), P(None, "dp", None)
    return jax.shard_map(
        step,
        mesh=mesh,
        in_specs=(P(("rep", "dp"), None, None, None),) * 3 + (all_of,) * 3 + (part,) * 6,
        out_specs=(P("rep", None, None),) * 3 + (P("rep", "dp", None),) * 6,
        check_vma=False,
    )
```

```python
import jax
import jax.numpy as jnp
from jax import lax
from jax.experimental import pallas as pl
from jax.experimental.pallas import tpu as pltpu
from jax.sharding import PartitionSpec as P

UP, DOWN, GATE = WEIGHTS = range(3)
N = 4
QUARTERS = range(N)
FLOWS = BOTH = range(2)
ALL = [(w, h) for h in FLOWS for w in WEIGHTS]
STRIDE = {"x": N * N, "y": N, "z": 1}
AXES = (("x", "y", "z"), ("y", "z", "x"), ("z", "x", "y"))
CHUNK_AXIS = ("y", "x", "x")
FAR_FIRST = (2, 1, 3)
OUTWARD = (0, -1, 1, 2)
NEAR = (-1, 1)
TILE = 16
BF, F32 = jnp.bfloat16, jnp.float32


def fori(n, body):
    lax.fori_loop(0, n, lambda i, c: (body(i), c)[1], 0)


def main_kernel(names, count, *refs):
    R = dict(zip(names, refs, strict=True))

    def three(name):
        return [R[name, w] for w in WEIGHTS]

    g, wt, mi, vi, W, mo, vo = (three(n) for n in ("g", "wt", "mi", "vi", "W", "mo", "vo"))
    own1, own2, r, ws, ms, vs, pieces = (three(n) for n in ("own1", "own2", "r", "ws", "ms", "vs", "pieces"))
    wl, mv = ([R[n, UP], R[n, DOWN], R[n, UP]] for n in ("wl", "mv"))
    tall = [R["tall", UP], R["tall", DOWN], R["tall", UP]]
    qa = {w: R["qa", w] for w in (UP, GATE)}
    gf = mo
    pb, bs, qb, bt, rb, fa, sa, ra, fc, sc, rc, tsc, tc, ub, uc, vc, nsend, nrecv = (
        R[n] for n in ("pb", "bs", "qb", "bt", "rb", "fa", "sa", "ra", "fc", "sc", "rc", "tsc", "tc", "ub", "uc", "vc", "nsend", "nrecv")
    )
    ua = sa
    sent, local, rec1, rec2, rec2b, rec3, recn, rech = (
        R[n] for n in ("sent", "local", "rec1", "rec2", "rec2b", "rec3", "recn", "rech")
    )
    tokens = iter(range(sent.shape[0]))
    leaving = []

    me = lax.axis_index("dp")
    co = {"x": me // STRIDE["x"], "y": me // STRIDE["y"] % N, "z": me % N}
    x, y, z = co["x"], co["y"], co["z"]

    def at(axis, off):
        return (co[axis] + off) % N

    def to(axis, off):
        return me + (at(axis, off) - co[axis]) * STRIDE[axis]

    def group(ref):
        sem = sent.at[next(tokens)]
        leaving.append((ref, sem))
        return sem

    def post(src, dst, ssem, rsem, device):
        pltpu.make_async_remote_copy(
            src_ref=src, dst_ref=dst, send_sem=ssem, recv_sem=rsem, device_id={"dp": device}, device_id_type=pl.DeviceIdType.MESH
        ).start()

    def send(src, dst, ssem, rsem, axis, off):
        post(src, dst, ssem, rsem, to(axis, off))

    def wait(ref, sem):
        pltpu.make_async_copy(ref, ref, sem).wait()

    def way(h):
        return 1 - 2 * h

    def offs(w, h):
        return (2, 1, -1, 0) if w == DOWN else (2, -way(h), way(h), 0)

    def term(w, h, q, c):
        if w == UP:
            return g[w].at[h, q, c]
        if w == DOWN:
            return g[w].at[h, c, q]
        cols = g[w].shape[-1] // 2
        return g[w].at[q // 2, c, h, :, pl.ds(pl.multiple_of(q % 2 * cols, 128), cols)]

    def tiles(n, body):
        fori(n // TILE, lambda i: body(pl.ds(pl.multiple_of(i * TILE, TILE), TILE)))

    def cut(w):
        rows, (_, pad, cols) = vi[w].shape[0], pieces[w].shape
        for q in QUARTERS:
            pieces[w][q] = tall[w][rows * q : rows * q + pad, 0:cols]

    def join(w, piece, cols):
        rows = vi[w].shape[0]
        for q in QUARTERS:
            tall[w][rows * q : rows * q + rows, 0:cols] = piece(q).astype(F32)[:rows]
        return tall[w][0 : N * rows, 0:cols].astype(BF)

    barrier = pltpu.get_barrier_semaphore()
    for axis in STRIDE:
        for off in NEAR:
            pl.semaphore_signal(barrier, inc=1, device_id={"dp": to(axis, off)}, device_id_type=pl.DeviceIdType.MESH)

    for which, buf in enumerate((own1, own2)):
        for w, h in ALL:
            q = at(AXES[w][0], way(h) * (1 - which))
            for k in QUARTERS:
                src = term(w, h, q, at(CHUNK_AXIS[w], offs(w, h)[k]))
                pltpu.make_async_copy(src, buf[w].at[h, k], local.at[which, w, h]).start()
    pl.semaphore_wait(barrier, len(STRIDE) * len(NEAR))

    left1 = [group(r[w]) for w in WEIGHTS]

    def phase1(i, w, h, k, src, off):
        send(src, r[w].at[i, h, k], left1[w], rec1.at[w, i, h, k], AXES[w][0], off)

    for i, (far, near) in enumerate(((2, 1), (-1, -1))):
        for k in QUARTERS:
            for w, h in ALL:
                s = way(h)
                src = term(w, h, at(AXES[w][0], far * s), at(CHUNK_AXIS[w], offs(w, h)[k]))
                phase1(i, w, h, k, src, near * s)

    def load_state(w):
        for i, (src, dst) in enumerate(((wt[w].at[:, x, y], wl[w]), (mi[w], mv[w].at[0]), (vi[w], mv[w].at[1]))):
            pltpu.make_async_copy(src, dst, local.at[2 + i // 2, w, i % 2]).start()

    load_state(UP)
    load_state(DOWN)
    for which, buf in enumerate((own1, own2)):
        for w, h in ALL:
            wait(buf[w].at[h], local.at[which, w, h])

    for k in QUARTERS:
        for w, h in ALL:
            wait(r[w].at[0, h, k], rec1.at[w, 0, h, k])

            def add(t, w=w, h=h, k=k):
                own1[w][h, k, t] = (own1[w][h, k, t].astype(F32) + r[w][0, h, k, t].astype(F32)).astype(BF)

            tiles(own1[w].shape[2], add)
            phase1(2, w, h, k, own1[w].at[h, k], way(h))

    for w in WEIGHTS:
        rows, (_, pad, cols) = vi[w].shape[0], ms[w].shape
        if w != GATE:
            n = N * rows
            tall[w][n : n + TILE, :] = jnp.zeros((TILE, tall[w].shape[1]), F32)
        for i, dst in enumerate((wl[w], mv[w].at[0], mv[w].at[1])):
            wait(dst, local.at[2 + i // 2, w, i % 2])
        for h in BOTH:
            for dst in (ms[w], vs[w]):
                dst[h, pad - 8 : pad] = jnp.zeros((8, cols), F32)

        def spread(i, w=w):
            for src, dst in ((mv[w][0, i], ms[w]), (mv[w][1, i], vs[w])):
                for h in BOTH:
                    dst[h, pl.ds(i, 1), :] = src[h : h + 1]

        fori(rows, spread)
        for h in BOTH:

            def widen(t, w=w, h=h):
                tall[w][t, :] = wl[w][h, t].astype(F32)

            tiles(N * rows, widen)
            src = pieces[w] if w != GATE else pieces[UP]
            cut(w if w != GATE else UP)
            ws[w][h] = src[z]
        if w == UP:
            load_state(GATE)

    def total(w, h, k, t):
        return own2[w][h, k, t].astype(F32) + r[w][1, h, k, t].astype(F32) + r[w][2, h, k, t].astype(F32)

    def cut_down(h, k):
        def put(t):
            tall[DOWN][t, :] = total(DOWN, h, k, t)

        tiles(own2[DOWN].shape[2], put)
        cut(DOWN)

    left2 = {w: group(qa[w]) for w in qa}
    left2b = group(qb)

    def phase2(i, w, h, off):
        send(own2[w].at[h, i], qa[w].at[h, i], left2[w], rec2.at[w // 2, h, i], AXES[w][1], off)

    def phase2b(i, h, k, off):
        send(bs.at[h, k, i], qb.at[h, k, i], left2b, rec2b.at[h, k, i], "z", off)

    for k in QUARTERS:
        for w, h in ALL:
            s = way(h)
            for i in (1, 2):
                wait(r[w].at[i, h, k], rec1.at[w, i, h, k])
            if w == DOWN:
                cut_down(h, k)
                pb[h, k] = pieces[w][z]
                for i, (far, near) in enumerate(((2, 1), (-1, -1))):
                    bs[h, k, i] = pieces[w][at("z", far * s)].astype(BF)
                    phase2b(i, h, k, near * s)
            elif k < 2:

                def put(t, w=w, h=h, k=k):
                    own2[w][h, k, t] = total(w, h, k, t).astype(BF)

                tiles(own2[w].shape[2], put)
                phase2(k, w, h, -s if k else s)

    for w in qa:
        for h in FLOWS:
            wait(qa[w].at[h, 0], rec2.at[w // 2, h, 0])

            def add2(t, w=w, h=h):
                own2[w][h, 2, t] = (total(w, h, 2, t) + qa[w][h, 0, t].astype(F32)).astype(BF)

            tiles(own2[w].shape[2], add2)
            phase2(2, w, h, way(h))
    for k in QUARTERS:
        for h in FLOWS:
            s = way(h)
            cut_down(h, k)
            wait(qb.at[h, k, 0], rec2b.at[h, k, 0])
            bs[h, k, 2] = (pieces[DOWN][at("z", s)] + qb[h, k, 0].astype(F32)).astype(BF)
            phase2b(2, h, k, s)

    left_a, left_c, left_b = group(ra), group(rc), group(rb)
    for w in qa:
        for h in BOTH:
            for i in (1, 2):
                wait(qa[w].at[h, i], rec2.at[w // 2, h, i])

            def total2(t, w=w, h=h):
                return total(w, h, 3, t) + qa[w][h, 1, t].astype(F32) + qa[w][h, 2, t].astype(F32)

            if w == UP:

                def put2(t, total2=total2):
                    tall[UP][t, :] = total2(t)

                tiles(own2[w].shape[2], put2)
                cut(UP)
                for q in QUARTERS:
                    sa[q, h] = pieces[UP][q].astype(BF)
                fa[h] = pieces[UP][z]
            else:
                n = fc.shape[1]
                for b in BOTH:

                    def put2(i, total2=total2, h=h, b=b, n=n):
                        v = total2(pl.ds(pl.multiple_of(b * n + i * TILE, TILE), TILE))
                        t = pl.ds(pl.multiple_of(i * TILE, TILE), TILE)
                        fc[2 * h + b, t] = v
                        sc[2 * h + b, t] = v.astype(BF)

                    fori(n // TILE, put2)
        for j in FAR_FIRST:
            if w == UP:
                send(sa.at[at("z", j)], ra.at[j - 1], left_a, rec3.at[0, j - 1], "z", j)
            else:
                send(sc.at[at("y", j)], rc.at[j - 1], left_c, rec3.at[1, j - 1], "y", j)
    for k in QUARTERS:
        for h in BOTH:
            for i in (1, 2):
                wait(qb.at[h, k, i], rec2b.at[h, k, i])
            v = pb[h, k] + qb[h, k, 1].astype(F32) + qb[h, k, 2].astype(F32)
            off = offs(DOWN, h)[k]
            if off:
                bt[h, k] = v.astype(BF)
                send(bt.at[h, k], rb.at[h, k], left_b, rec3.at[2 + h, k], "x", off)
            else:
                pb[h, k] = v

    def fold(v):
        v = jnp.sum(v * v, axis=0, keepdims=True)
        out = v[:, 0:128]
        for i in range(128, v.shape[1], 128):
            out = out + v[:, i : i + 128]
        nsend[...] = nsend[...] + out

    def valid(n, v):
        return jnp.where(lax.broadcasted_iota(jnp.int32, v.shape, 0) < n, v, 0.0)

    def rounded(own, others):
        for o in others:
            own = own + o.astype(F32)
        return own.astype(BF).astype(F32)

    others = range(len(FAR_FIRST))
    half = tsc.shape[-1]
    nsend[...] = jnp.zeros(nsend.shape, F32)
    for j in others:
        wait(rc.at[j], rec3.at[1, j])

    def last_c(t):
        v = rounded(fc[y, t], [rc[j, t] for j in others])
        tall[UP][t, 0:half] = v
        fold(v)

    tiles(fc.shape[1], last_c)
    cut(GATE)
    for q in QUARTERS:
        tsc[q] = pieces[GATE][q].astype(BF)
    tc[z] = tsc[z]
    left = group(tc.at[0:3])
    for j in FAR_FIRST:
        send(tsc.at[at("z", j)], tc.at[z], left, rech.at[0, j - 1], "z", j)
    for j in others:
        wait(ra.at[j], rec3.at[0, j])
    (gone,) = [i for i, (_, sem) in enumerate(leaving) if sem is left_a]
    wait(*leaving.pop(gone))
    for h in BOTH:
        v = rounded(fa[h], [ra[j, h] for j in others])
        gf[UP][h] = v
        fold(valid(vi[UP].shape[0], v))
    for h in BOTH:
        for k in others:
            wait(rb.at[h, k], rec3.at[2 + h, k])
        v = rounded(pb[h, 3], [rb[h, k] for k in others])
        gf[DOWN][h] = v
        fold(valid(vi[DOWN].shape[0], v))

    devices = nrecv.shape[0]
    nrecv[me] = nsend[...]
    left = group(nrecv.at[1:devices])
    away = [(min(i, N - i), i) for i in QUARTERS]
    for _, i, j, k in sorted((a + b + c, i, j, k) for a, i in away for b, j in away for c, k in away)[:0:-1]:
        post(nsend, nrecv.at[me], left, recn.at[0], to("x", i) + to("y", j) + to("z", k) - 2 * me)
    for j in FAR_FIRST:
        wait(tc.at[at("z", -j)], rech.at[0, j - 1])
    wait(nrecv.at[1:devices], recn.at[0])
    squares = jnp.sum(jnp.sum(nrecv[...], axis=0), axis=1, keepdims=True)
    factor = jnp.minimum(1.0, 0.5 * lax.rsqrt(squares / count + 1e-30))
    for q in QUARTERS:
        gf[GATE][q // 2, :, half * (q % 2) : half * (q % 2 + 1)] = tc[q].astype(F32)

    def adamw(w, h):
        gc = gf[w][h] * factor
        m = 0.9 * ms[w][h] + 0.1 * gc
        v = 0.95 * vs[w][h] + 0.05 * gc * gc
        mo[w][h] = m
        vo[w][h] = v
        step = m * lax.rsqrt(v + 1e-8) + 0.1 * ws[w][h]
        return (ws[w][h] - 0.02 * step).astype(BF)

    def spread_out(i, axis, ref, first):
        left = group(first)
        for j in FAR_FIRST:
            send(ref(co[axis]), ref(co[axis]), left, rech.at[i, j], axis, j)

    def arrived(i, axis, ref, j):
        wait(ref(at(axis, -j)), rech.at[i, j])

    for h in BOTH:
        new = adamw(GATE, h)
        vc[2 * h] = new[:, :half]
        vc[2 * h + 1] = new[:, half:]
    uc[y, z] = vc[z]
    left = group(uc.at[0:3])
    left0 = group(uc.at[0, 0:3])
    for j in (*FAR_FIRST, 0):
        for i in (*FAR_FIRST, 0):
            if i or j:
                src, device = vc.at[at("z", i)], to("y", j) + to("z", i) - me
                post(src, uc.at[y, z], left if j else left0, rech.at[N, j], device)
    for h in BOTH:
        ua[z, h] = adamw(UP, h)
        spread_out(1 + h, "z", lambda p: ua.at[p, h], ua.at[0:3, 0])
    for h in BOTH:
        ub[z, x, h] = adamw(DOWN, h)
    spread_out(3, "x", lambda p: ub.at[z, p], ub.at[0, 0:3])

    class Ring:
        def __init__(self, ref, sub, left, recv, axis):
            self.ref, self.sub, self.left, self.recv, self.axis = ref, sub, left, recv, axis

        def half(self, p, h):
            return self.ref(p).at[self.sub(h)]

        def own(self, h):
            for d in BOTH:
                ref = self.half(0, h)
                send(ref, ref, self.left, self.recv(d, h), self.axis, way(d))

        def owns(self):
            for h in BOTH:
                self.own(h)

        def pass_on(self):
            for d in BOTH:
                ref = self.half(NEAR[d], d)
                wait(ref, self.recv(d, d))
                send(ref, ref, self.left, self.recv(2, d), self.axis, way(d))

        def near(self, d):
            wait(self.half(NEAR[d], 1 - d), self.recv(d, 1 - d))

        def far(self):
            for d in BOTH:
                wait(self.half(2, d), self.recv(2, d))

    def one(h):
        return h

    def two(h):
        return pl.ds(2 * h, 2)

    def outer_ring(w, i, left):
        a, c = AXES[w][0], CHUNK_AXIS[w]
        return Ring(
            lambda p: W[w].at[at(a, p), at(c, OUTWARD[i])],
            two if w == GATE else one,
            left,
            lambda u, v: rec1.at[w, u, v, i],
            a,
        )

    left_o = [group(W[w].at[0:3]) for w in WEIGHTS]
    outer = [[outer_ring(w, i, left_o[w]) for i in QUARTERS] for w in WEIGHTS]
    left_z, left_y, left_x = group(ub.at[0:3]), group(W[UP].at[0, 0:3]), group(W[GATE].at[0, 0:3])
    zring = [
        Ring(lambda p, off=off: ub.at[at("z", p), at("x", off)], one, left_z, lambda u, v, i=i: rec2b.at[v, i, u], "z")
        for i, off in enumerate(OUTWARD)
    ]
    yring = Ring(lambda p: W[UP].at[x, at("y", p)], one, left_y, lambda u, v: rec2.at[0, v, u], "y")
    xring = Ring(lambda p: W[GATE].at[z, at("x", p)], two, left_x, lambda u, v: rec2.at[1, v, u], "x")

    zring[0].owns()
    for i, off in enumerate(OUTWARD):
        if off:
            arrived(3, "x", lambda p: ub.at[z, p], -off % N)
            zring[i].owns()
    for h in BOTH:
        for j in FAR_FIRST:
            arrived(1 + h, "z", lambda p: ua.at[p, h], j)
        W[UP][x, y, h] = join(UP, lambda q: ua[q, h], tall[UP].shape[1])
        yring.own(h)
        outer[UP][0].own(h)
    zring[0].pass_on()
    for j in QUARTERS:
        ref = uc.at[at("y", -j)]
        wait(ref if j else ref.at[0:3], rech.at[N, j])
    for b in QUARTERS:
        W[GATE][z, x, b] = join(GATE, lambda q: uc[b, q], half)
    xring.owns()
    outer[GATE][0].owns()
    zring[1].pass_on()
    zring[2].pass_on()
    yring.pass_on()
    for d in BOTH:
        yring.near(d)
        if not d:
            outer[UP][1].owns()
    zring[3].pass_on()
    xring.pass_on()
    for d in BOTH:
        xring.near(d)
        if not d:
            outer[GATE][1].owns()
    for i in QUARTERS:
        for d in BOTH:
            zring[i].near(d)
        zring[i].far()
        c = at("x", OUTWARD[i])
        for h in BOTH:
            W[DOWN][y, c, h] = join(DOWN, lambda q: ub[q, c, h], tall[DOWN].shape[1])
        outer[DOWN][i].owns()
    outer[UP][2].owns()
    outer[GATE][2].owns()
    yring.far()
    outer[UP][3].owns()
    xring.far()
    outer[GATE][3].owns()
    for i in QUARTERS:
        for w in WEIGHTS:
            outer[w][i].pass_on()
    for i in QUARTERS:
        for w in WEIGHTS:
            for d in BOTH:
                outer[w][i].near(d)
            outer[w][i].far()
    for ref, sem in leaving:
        wait(ref, sem)


def write_kernel(names, *refs):
    R = dict(zip(names, refs, strict=True))
    W = [R["W", w] for w in WEIGHTS]
    out = [R["out", w] for w in WEIGHTS]
    half = W[GATE].shape[-1]
    copies = []
    for p in QUARTERS:
        for h in BOTH:
            cols, two = pl.ds(half * (p % 2), half), pl.ds(2 * h, 2)
            pairs = (
                (W[UP].at[p, :, h], out[UP].at[h, p]),
                (W[DOWN].at[p, :, h], out[DOWN].at[h, :, p]),
                (W[GATE].at[p, two], out[GATE].at[p // 2, two, :, :, cols]),
            )
            copies += [pltpu.make_async_copy(*pair, R["sem"].at[w, p, h]) for w, pair in enumerate(pairs)]
    for c in copies:
        c.start()
    for w in WEIGHTS:

        def gather(i, w=w):
            for n in "mv":
                for h in BOTH:
                    R[n + "b", w][i, h : h + 1] = R[n + "o", w][h, pl.ds(i, 1), :]

        fori(R["mb", w].shape[0], gather)
        for i, n in enumerate("mv"):
            copies.append(pltpu.make_async_copy(R[n + "b", w], R[n + "out", w], R["small"].at[i, w]))
            copies[-1].start()
    for c in copies:
        c.wait()


def call(kernel, ins, outs, scratch, place_in, place_out, **params):
    names = (*ins, *outs, *scratch)
    got = pl.pallas_call(
        lambda *refs: kernel(names, *refs),
        out_shape=list(outs.values()),
        in_specs=[pl.BlockSpec(memory_space=place_in)] * len(ins),
        out_specs=[pl.BlockSpec(memory_space=place_out)] * len(outs),
        scratch_shapes=list(scratch.values()),
        name=kernel.__name__,
        compiler_params=pltpu.CompilerParams(**params),
    )(*ins.values())
    return dict(zip(outs, got, strict=True))


def by_weight(**of):
    return {(n, w): t for n, ts in of.items() for w, t in zip(WEIGHTS, ts)}


def solution(mesh):
    def step(*arrays):
        terms, weights, m, v = ([arrays[i + j] for j in (1, 2, 0)] for i in (0, 3, 6, 9))
        (rows, ff), (rows_d, d) = m[0].shape[1:], m[1].shape[1:]
        half, n, n_d = ff // 2, N * rows, N * rows_d
        full = ((2, N, N, n, ff), (2, N, N, n_d, d), (2, N, N, n, ff))
        g = [t.reshape(s) for t, s in zip(terms, (*full[:2], (2, N, 2, 2 * n, ff)))]
        state = [[pltpu.with_memory_space_constraint(a.transpose(1, 0, 2), pltpu.HBM) for a in t] for t in (m, v)]
        weights = [a.reshape(s) for a, s in zip(weights, full)]
        ins = by_weight(g=g, wt=weights, mi=state[0], vi=state[1])

        vm, dma = pltpu.VMEM, pltpu.SemaphoreType.DMA
        pad, pad_d = 16, 32
        chunk = ((n, ff), (n_d, d), (2 * n, half))
        own = ((2, pad, ff), (2, pad_d, d), (2, pad, ff))
        pieces = [vm((N, *s), F32) for s in ((pad, ff), (pad_d, d), (pad, half))]
        scratch = by_weight(
            own1=[vm((2, N, *c), BF) for c in chunk],
            own2=[vm((2, N, *c), BF) for c in chunk],
            r=[vm((3, 2, N, *c), BF) for c in chunk],
            ws=[vm(s, F32) for s in own],
            ms=[vm(s, F32) for s in own],
            vs=[vm(s, F32) for s in own],
            pieces=pieces,
            wl=[vm((2, *c), BF) for c in chunk[:2]],
            mv=[vm((2, *a.shape), F32) for a in state[0][:2]],
            tall=[vm((n + TILE, ff), F32), vm((n_d + TILE, d), F32)],
        )
        scratch |= {("qa", w): vm((2, 3, *chunk[w]), BF) for w in (UP, GATE)}
        scratch |= dict(
            pb=vm((2, N, pad_d, d), F32),
            bs=vm((2, N, 3, pad_d, d), BF),
            qb=vm((2, N, 3, pad_d, d), BF),
            bt=vm((2, 3, pad_d, d), BF),
            rb=vm((2, 3, pad_d, d), BF),
            fa=vm((2, pad, ff), F32),
            sa=vm((N, 2, pad, ff), BF),
            ra=vm((3, 2, pad, ff), BF),
            fc=vm((N, n, half), F32),
            sc=vm((N, n, half), BF),
            rc=vm((3, n, half), BF),
            tsc=vm((N, pad, half), BF),
            tc=vm((N, pad, half), BF),
            ub=vm((N, N, 2, pad_d, d), BF),
            uc=vm((N, N, pad, half), BF),
            vc=vm((N, pad, half), BF),
            nsend=vm((1, 128), F32),
            nrecv=vm((N**3, 1, 128), F32),
            sent=dma((24,)),
            local=dma((N, 3, 2)),
            rec1=dma((3, 3, 2, N)),
            rec2=dma((2, 2, 3)),
            rec2b=dma((2, N, 3)),
            rec3=dma((N, 3)),
            recn=dma((1,)),
            rech=dma((N + 1, N)),
        )
        outs = by_weight(
            W=[jax.ShapeDtypeStruct(s, BF) for s in ((N, N, 2, n, ff), (N, N, 2, n_d, d), (N, N, N, n, half))],
            mo=[jax.ShapeDtypeStruct(s, F32) for s in own],
            vo=[jax.ShapeDtypeStruct(s, F32) for s in own],
        )
        count = float(N**3 * sum(a.size for a in m))

        def main(names, *refs):
            main_kernel(names, count, *refs)

        got = call(main, ins, outs, scratch, pltpu.HBM, vm, collective_id=0, has_side_effects=True, vmem_limit_bytes=36900000)
        small = [jax.ShapeDtypeStruct(a.shape, F32) for a in state[0]]
        outs = by_weight(out=[jax.ShapeDtypeStruct(s, BF) for s in full], mout=small, vout=small)
        scratch = by_weight(mb=[vm(a.shape, F32) for a in small], vb=[vm(a.shape, F32) for a in small])
        scratch |= dict(sem=dma((3, N, 2)), small=dma((2, 3)))
        new = call(write_kernel, got, outs, scratch, vm, pltpu.HBM, vmem_limit_bytes=2000000)
        back = (GATE, UP, DOWN)
        whole = [new["out", w].reshape(2, -1, full[w][-1]) for w in back]
        return (*whole, *(new[n, w].transpose(1, 0, 2) for n in ("mout", "vout") for w in back))

    all_of, part = P(None, None, None), P(None, "dp", None)
    return jax.shard_map(
        step,
        mesh=mesh,
        in_specs=(P(("rep", "dp"), None, None, None),) * 3 + (all_of,) * 3 + (part,) * 6,
        out_specs=(P("rep", None, None),) * 3 + (P("rep", "dp", None),) * 6,
        check_vma=False,
    )
```

```python
import jax
import jax.numpy as jnp
from jax import lax
from jax.experimental import pallas as pl
from jax.experimental.pallas import tpu as pltpu
from jax.sharding import PartitionSpec as P

UP, DOWN, GATE = WEIGHTS = range(3)
N = 4
QUARTERS = range(N)
FLOWS = BOTH = range(2)
ALL = [(w, h) for h in FLOWS for w in WEIGHTS]
STRIDE = {"x": N * N, "y": N, "z": 1}
AXES = (("x", "y", "z"), ("y", "z", "x"), ("z", "x", "y"))
CHUNK_AXIS = ("y", "x", "x")
FAR_FIRST = (2, 1, 3)
OUTWARD = (0, -1, 1, 2)
NEAR = (-1, 1)
TILE = 16
BF, F32 = jnp.bfloat16, jnp.float32


def fori(n, body):
    lax.fori_loop(0, n, lambda i, c: (body(i), c)[1], 0)


def main_kernel(names, count, *refs):
    R = dict(zip(names, refs, strict=True))

    def three(name):
        return [R[name, w] for w in WEIGHTS]

    g, wt, mi, vi, W, mo, vo = (three(n) for n in ("g", "wt", "mi", "vi", "W", "mo", "vo"))
    own1, own2, r, ws, ms, vs, pieces = (three(n) for n in ("own1", "own2", "r", "ws", "ms", "vs", "pieces"))
    wl, mv = ([R[n, UP], R[n, DOWN], R[n, UP]] for n in ("wl", "mv"))
    tall = [R["tall", UP], R["tall", DOWN], R["tall", UP]]
    qa = {w: R["qa", w] for w in (UP, GATE)}
    gf = mo
    pb, bs, qb, bt, rb, fa, sa, ra, fc, sc, rc, tsc, tc, ub, uc, vc, nsend, nrecv = (
        R[n] for n in ("pb", "bs", "qb", "bt", "rb", "fa", "sa", "ra", "fc", "sc", "rc", "tsc", "tc", "ub", "uc", "vc", "nsend", "nrecv")
    )
    ua = sa
    sent, local, rec1, rec2, rec2b, rec3, recn, rech = (
        R[n] for n in ("sent", "local", "rec1", "rec2", "rec2b", "rec3", "recn", "rech")
    )
    tokens = iter(range(sent.shape[0]))
    leaving = []

    me = lax.axis_index("dp")
    co = {"x": me // STRIDE["x"], "y": me // STRIDE["y"] % N, "z": me % N}
    x, y, z = co["x"], co["y"], co["z"]

    def at(axis, off):
        return (co[axis] + off) % N

    def to(axis, off):
        return me + (at(axis, off) - co[axis]) * STRIDE[axis]

    def group(ref):
        sem = sent.at[next(tokens)]
        leaving.append((ref, sem))
        return sem

    def post(src, dst, ssem, rsem, device):
        pltpu.make_async_remote_copy(
            src_ref=src, dst_ref=dst, send_sem=ssem, recv_sem=rsem, device_id={"dp": device}, device_id_type=pl.DeviceIdType.MESH
        ).start()

    def send(src, dst, ssem, rsem, axis, off):
        post(src, dst, ssem, rsem, to(axis, off))

    def wait(ref, sem):
        pltpu.make_async_copy(ref, ref, sem).wait()

    def way(h):
        return 1 - 2 * h

    def offs(w, h):
        return (2, 1, -1, 0) if w == DOWN else (2, -way(h), way(h), 0)

    def term(w, h, q, c):
        if w == UP:
            return g[w].at[h, q, c]
        if w == DOWN:
            return g[w].at[:, c, q, :, down_cols(h)]
        cols = g[w].shape[-1] // 2
        return g[w].at[q // 2, c, h, :, pl.ds(pl.multiple_of(q % 2 * cols, 128), cols)]

    def rows_of(i):
        return pl.ds(pl.multiple_of(i * TILE, TILE), TILE)

    def tiles(w, body):
        n = own1[w].shape[-2] // TILE
        if w == DOWN:
            fori(2 * n, lambda i: body((i // n, rows_of(i % n))))
        else:
            fori(n, lambda i: body((rows_of(i),)))

    def down_cols(h):
        cols = own1[DOWN].shape[-1]
        return pl.ds(h * cols, cols)

    def cut(w, h):
        rows, cols = vi[w].shape[0], pieces[w].shape[-1]
        for q in QUARTERS:
            pieces[w][q, rows * h : rows * (h + 1)] = tall[w][rows * q : rows * (q + 1), 0:cols]

    def join(w, h):
        rows, cols = vi[w].shape[0], pieces[w].shape[-1]
        for q in QUARTERS:
            tall[w][rows * q : rows * (q + 1), 0:cols] = pieces[w][q, rows * h : rows * (h + 1)]
        return tall[w][0 : N * rows, 0:cols].astype(BF)

    barrier = pltpu.get_barrier_semaphore()
    for axis in STRIDE:
        for off in NEAR:
            pl.semaphore_signal(barrier, inc=1, device_id={"dp": to(axis, off)}, device_id_type=pl.DeviceIdType.MESH)

    for which, buf in enumerate((own1, own2)):
        for w, h in ALL:
            q = at(AXES[w][0], way(h) * (1 - which))
            for k in QUARTERS:
                src = term(w, h, q, at(CHUNK_AXIS[w], offs(w, h)[k]))
                pltpu.make_async_copy(src, buf[w].at[h, k], local.at[which, w, h]).start()
    pl.semaphore_wait(barrier, len(STRIDE) * len(NEAR))

    left1 = [group(r[w]) for w in WEIGHTS]

    def phase1(i, w, h, k, src, off):
        send(src, r[w].at[i, h, k], left1[w], rec1.at[w, i, h, k], AXES[w][0], off)

    for i, (far, near) in enumerate(((2, 1), (-1, -1))):
        for k in QUARTERS:
            for w, h in ALL:
                s = way(h)
                src = term(w, h, at(AXES[w][0], far * s), at(CHUNK_AXIS[w], offs(w, h)[k]))
                phase1(i, w, h, k, src, near * s)

    def load_state(w):
        for i, (src, dst) in enumerate(((wt[w].at[:, x, y], wl[w]), (mi[w], mv[w].at[0]), (vi[w], mv[w].at[1]))):
            pltpu.make_async_copy(src, dst, local.at[2 + i // 2, w, i % 2]).start()

    load_state(UP)
    load_state(DOWN)
    for which, buf in enumerate((own1, own2)):
        for w, h in ALL:
            wait(buf[w].at[h], local.at[which, w, h])

    for k in QUARTERS:
        for w, h in ALL:
            wait(r[w].at[0, h, k], rec1.at[w, 0, h, k])

            def add(t, w=w, h=h, k=k):
                t = (h, k, *t)
                own1[w][t] = (own1[w][t].astype(F32) + r[w][(0, *t)].astype(F32)).astype(BF)

            tiles(w, add)
            phase1(2, w, h, k, own1[w].at[h, k], way(h))

    pieces[GATE][...] = jnp.zeros(pieces[GATE].shape, F32)
    for w in WEIGHTS:
        rows = vi[w].shape[0]
        for i, dst in enumerate((wl[w], mv[w].at[0], mv[w].at[1])):
            wait(dst, local.at[2 + i // 2, w, i % 2])

        def spread(i, w=w, rows=rows):
            for src, dst in ((mv[w][0, i], ms[w]), (mv[w][1, i], vs[w])):
                for h in BOTH:
                    dst[pl.ds(rows * h + i, 1), :] = src[h : h + 1]

        fori(rows, spread)
        v = DOWN if w == DOWN else UP
        for cols in [down_cols(c) for c in BOTH] if w == DOWN else [slice(None)]:
            for h in BOTH:

                def widen(i, w=w, h=h, v=v, cols=cols):
                    t = rows_of(i)
                    tall[v][t, :] = wl[w][h, t, cols].astype(F32)

                fori(N * rows // TILE, widen)
                cut(v, h)
            ws[w][:, cols] = pieces[v][z]
        if w == UP:
            load_state(GATE)

    def total(w, h, k, t):
        t = (h, k, *t)
        return own2[w][t].astype(F32) + r[w][(1, *t)].astype(F32) + r[w][(2, *t)].astype(F32)

    def cut_down(h, k):
        n = own2[DOWN].shape[-2]
        for layer in BOTH:

            def put(i, layer=layer):
                t = rows_of(i)
                tall[DOWN][t, :] = total(DOWN, h, k, (layer, t))

            fori(n // TILE, put)
            cut(DOWN, layer)

    left2 = {w: group(qa[w]) for w in qa}
    left2b = group(qb)

    def phase2(i, w, h, off):
        send(own2[w].at[h, i], qa[w].at[h, i], left2[w], rec2.at[w // 2, h, i], AXES[w][1], off)

    def phase2b(i, h, k, off):
        send(bs.at[h, k, i], qb.at[h, k, i], left2b, rec2b.at[h, k, i], "z", off)

    for k in QUARTERS:
        for w, h in ALL:
            s = way(h)
            for i in (1, 2):
                wait(r[w].at[i, h, k], rec1.at[w, i, h, k])
            if w == DOWN:
                cut_down(h, k)
                pb[h, k] = pieces[w][z]
                for i, (far, near) in enumerate(((2, 1), (-1, -1))):
                    bs[h, k, i] = pieces[w][at("z", far * s)].astype(BF)
                    phase2b(i, h, k, near * s)
            elif k < 2:

                def put(t, w=w, h=h, k=k):
                    own2[w][(h, k, *t)] = total(w, h, k, t).astype(BF)

                tiles(w, put)
                phase2(k, w, h, -s if k else s)

    for w in qa:
        for h in FLOWS:
            wait(qa[w].at[h, 0], rec2.at[w // 2, h, 0])

            def add2(t, w=w, h=h):
                own2[w][(h, 2, *t)] = (total(w, h, 2, t) + qa[w][(h, 0, *t)].astype(F32)).astype(BF)

            tiles(w, add2)
            phase2(2, w, h, way(h))
    for k in QUARTERS:
        for h in FLOWS:
            s = way(h)
            cut_down(h, k)
            wait(qb.at[h, k, 0], rec2b.at[h, k, 0])
            bs[h, k, 2] = (pieces[DOWN][at("z", s)] + qb[h, k, 0].astype(F32)).astype(BF)
            phase2b(2, h, k, s)

    left_a, left_c, left_b = group(ra), group(rc), group(rb)
    for w in qa:
        for h in BOTH:
            for i in (1, 2):
                wait(qa[w].at[h, i], rec2.at[w // 2, h, i])

            def total2(t, w=w, h=h):
                return total(w, h, 3, t) + qa[w][(h, 1, *t)].astype(F32) + qa[w][(h, 2, *t)].astype(F32)

            if w == UP:

                def put2(t, total2=total2):
                    tall[UP][(*t, slice(None))] = total2(t)

                tiles(w, put2)
                cut(UP, h)
            else:
                n = fc.shape[1]
                for b in BOTH:

                    def put2(i, total2=total2, h=h, b=b, n=n):
                        v = total2((pl.ds(pl.multiple_of(b * n + i * TILE, TILE), TILE),))
                        t = rows_of(i)
                        fc[2 * h + b, t] = v
                        sc[2 * h + b, t] = v.astype(BF)

                    fori(n // TILE, put2)
        if w == UP:
            for q in QUARTERS:
                sa[q] = pieces[UP][q].astype(BF)
            fa[...] = pieces[UP][z]
        for j in FAR_FIRST:
            if w == UP:
                send(sa.at[at("z", j)], ra.at[j - 1], left_a, rec3.at[0, j - 1], "z", j)
            else:
                send(sc.at[at("y", j)], rc.at[j - 1], left_c, rec3.at[1, j - 1], "y", j)
    for k in QUARTERS:
        for h in BOTH:
            for i in (1, 2):
                wait(qb.at[h, k, i], rec2b.at[h, k, i])
            v = pb[h, k] + qb[h, k, 1].astype(F32) + qb[h, k, 2].astype(F32)
            off = offs(DOWN, h)[k]
            if off:
                bt[h, k] = v.astype(BF)
                send(bt.at[h, k], rb.at[h, k], left_b, rec3.at[2 + h, k], "x", off)
            else:
                pb[h, k] = v

    def fold(v):
        v = jnp.sum(v * v, axis=0, keepdims=True)
        out = v[:, 0:128]
        for i in range(128, v.shape[1], 128):
            out = out + v[:, i : i + 128]
        nsend[...] = nsend[...] + out

    def rounded(own, others):
        for o in others:
            own = own + o.astype(F32)
        return own.astype(BF).astype(F32)

    others = range(len(FAR_FIRST))
    half = tsc.shape[-1]
    nsend[...] = jnp.zeros(nsend.shape, F32)
    for j in others:
        wait(rc.at[j], rec3.at[1, j])

    def last_c(i):
        t = rows_of(i)
        v = rounded(fc[y, t], [rc[j, t] for j in others])
        tall[UP][t, 0:half] = v
        fold(v)

    fori(fc.shape[1] // TILE, last_c)
    cut(GATE, 0)
    for q in QUARTERS:
        tsc[q] = pieces[GATE][q].astype(BF)
    tc[z] = tsc[z]
    left = group(tc.at[0:3])
    for j in FAR_FIRST:
        send(tsc.at[at("z", j)], tc.at[z], left, rech.at[0, j - 1], "z", j)
    for j in others:
        wait(ra.at[j], rec3.at[0, j])
    (gone,) = [i for i, (_, sem) in enumerate(leaving) if sem is left_a]
    wait(*leaving.pop(gone))
    v = rounded(fa[...], [ra[j] for j in others])
    gf[UP][...] = v
    fold(v)
    for h in BOTH:
        for k in others:
            wait(rb.at[h, k], rec3.at[2 + h, k])
        v = rounded(pb[h, 3], [rb[h, k] for k in others])
        gf[DOWN][:, down_cols(h)] = v
        fold(v)

    devices = nrecv.shape[0]
    nrecv[me] = nsend[...]
    left = group(nrecv.at[1:devices])
    away = [(min(i, N - i), i) for i in QUARTERS]
    for _, i, j, k in sorted((a + b + c, i, j, k) for a, i in away for b, j in away for c, k in away)[:0:-1]:
        post(nsend, nrecv.at[me], left, recn.at[0], to("x", i) + to("y", j) + to("z", k) - 2 * me)
    for j in FAR_FIRST:
        wait(tc.at[at("z", -j)], rech.at[0, j - 1])
    wait(nrecv.at[1:devices], recn.at[0])
    squares = jnp.sum(jnp.sum(nrecv[...], axis=0), axis=1, keepdims=True)
    factor = jnp.minimum(1.0, 0.5 * lax.rsqrt(squares / count + 1e-30))
    rows = vi[GATE].shape[0]

    def gate_part(q):
        return slice(rows * (q // 2), rows * (q // 2 + 1)), slice(half * (q % 2), half * (q % 2 + 1))

    for q in QUARTERS:
        gf[GATE][gate_part(q)] = tc[q].astype(F32)[:rows]

    def adamw(w):
        gc = gf[w][...] * factor
        m = 0.9 * ms[w][...] + 0.1 * gc
        v = 0.95 * vs[w][...] + 0.05 * gc * gc
        mo[w][...] = m
        vo[w][...] = v
        step = m * lax.rsqrt(v + 1e-8) + 0.1 * ws[w][...]
        return ws[w][...] - 0.02 * step

    def spread_out(i, axis, ref, first):
        left = group(first)
        for j in FAR_FIRST:
            send(ref(co[axis]), ref(co[axis]), left, rech.at[i, j], axis, j)

    def arrived(i, axis, ref, j):
        wait(ref(at(axis, -j)), rech.at[i, j])

    pieces[UP][0] = adamw(GATE)
    for q in QUARTERS:
        pieces[GATE][q, 0:rows] = pieces[UP][(0, *gate_part(q))]
        vc[q] = pieces[GATE][q].astype(BF)
    uc[z] = vc[z]
    left = group(uc.at[0:3])
    for j in FAR_FIRST:
        send(vc.at[at("z", j)], uc.at[z], left, rech.at[N, j], "z", j)
    ua[z] = adamw(UP).astype(BF)
    spread_out(1, "z", lambda p: ua.at[p], ua.at[0:3])
    ub[z, x] = adamw(DOWN).astype(BF)
    spread_out(3, "x", lambda p: ub.at[z, p], ub.at[0, 0:3])

    class Ring:
        def __init__(self, ref, sub, left, recv, axis):
            self.ref, self.sub, self.left, self.recv, self.axis = ref, sub, left, recv, axis

        def half(self, p, h):
            return self.ref(p).at[self.sub(h)]

        def own(self, h):
            for d in BOTH:
                ref = self.half(0, h)
                send(ref, ref, self.left, self.recv(d, h), self.axis, way(d))

        def owns(self):
            for h in BOTH:
                self.own(h)

        def pass_on(self):
            for d in BOTH:
                ref = self.half(NEAR[d], d)
                wait(ref, self.recv(d, d))
                send(ref, ref, self.left, self.recv(2, d), self.axis, way(d))

        def near(self, d):
            wait(self.half(NEAR[d], 1 - d), self.recv(d, 1 - d))

        def far(self):
            for d in BOTH:
                wait(self.half(2, d), self.recv(2, d))

    def one(h):
        return h

    def two(h):
        return pl.ds(2 * h, 2)

    def outer_ring(w, i, left):
        a, c = AXES[w][0], CHUNK_AXIS[w]
        return Ring(
            lambda p: W[w].at[at(a, p), at(c, OUTWARD[i])],
            two if w == GATE else one,
            left,
            lambda u, v: rec1.at[w, u, v, i],
            a,
        )

    left_o = [group(W[w].at[0:3]) for w in WEIGHTS]
    outer = [[outer_ring(w, i, left_o[w]) for i in QUARTERS] for w in WEIGHTS]
    left_z, left_y, left_x = group(ub.at[0:3]), group(W[UP].at[0, 0:3]), group(W[GATE].at[0, 0:3])
    zring = [
        Ring(lambda p, off=off: ub.at[at("z", p), at("x", off)], lambda h: (slice(None), down_cols(h)), left_z, lambda u, v, i=i: rec2b.at[v, i, u], "z")
        for i, off in enumerate(OUTWARD)
    ]
    yring = Ring(lambda p: W[UP].at[x, at("y", p)], one, left_y, lambda u, v: rec2.at[0, v, u], "y")
    xring = Ring(lambda p: W[GATE].at[z, at("x", p)], two, left_x, lambda u, v: rec2.at[1, v, u], "x")

    zring[0].owns()
    for j in FAR_FIRST:
        arrived(N, "z", lambda p: uc.at[p], j)
    for q in QUARTERS:
        pieces[GATE][q] = uc[q].astype(F32)
    W[GATE][z, x, y] = join(GATE, 0)
    spread_out(N + 1, "y", lambda p: W[GATE].at[z, x, p], W[GATE].at[0, 0, 0:3])
    for i, off in enumerate(OUTWARD):
        if off:
            arrived(3, "x", lambda p: ub.at[z, p], -off % N)
            zring[i].owns()
    for j in FAR_FIRST:
        arrived(1, "z", lambda p: ua.at[p], j)
    for q in QUARTERS:
        pieces[UP][q] = ua[q].astype(F32)
    for h in BOTH:
        W[UP][x, y, h] = join(UP, h)
        yring.own(h)
        outer[UP][0].own(h)
    zring[0].pass_on()
    for j in FAR_FIRST:
        arrived(N + 1, "y", lambda p: W[GATE].at[z, x, p], j)
    xring.owns()
    for i in QUARTERS:
        if i:
            zring[i].pass_on()
    outer[GATE][0].owns()
    yring.pass_on()
    for d in BOTH:
        yring.near(d)
    outer[UP][1].owns()
    for i in QUARTERS:
        for d in BOTH:
            zring[i].near(d)
        zring[i].far()
        c = at("x", OUTWARD[i])
        for d in BOTH:
            for q in QUARTERS:
                pieces[DOWN][q] = ub[q, c, :, down_cols(d)].astype(F32)
            for h in BOTH:
                W[DOWN][y, c, h, :, down_cols(d)] = join(DOWN, h)
        outer[DOWN][i].owns()
    xring.pass_on()
    for d in BOTH:
        xring.near(d)
    outer[UP][2].owns()
    outer[GATE][1].owns()
    outer[GATE][2].owns()
    yring.far()
    outer[UP][3].owns()
    xring.far()
    outer[GATE][3].owns()
    for i in QUARTERS:
        for w in WEIGHTS:
            outer[w][i].pass_on()
    for i in QUARTERS:
        for w in WEIGHTS:
            for d in BOTH:
                outer[w][i].near(d)
            outer[w][i].far()
    for ref, sem in leaving:
        wait(ref, sem)


def write_kernel(names, *refs):
    R = dict(zip(names, refs, strict=True))
    W = [R["W", w] for w in WEIGHTS]
    out = [R["out", w] for w in WEIGHTS]
    half = W[GATE].shape[-1]
    copies = []
    for p in QUARTERS:
        for h in BOTH:
            cols, two = pl.ds(half * (p % 2), half), pl.ds(2 * h, 2)
            pairs = (
                (W[UP].at[p, :, h], out[UP].at[h, p]),
                (W[DOWN].at[p, :, h], out[DOWN].at[h, :, p]),
                (W[GATE].at[p, two], out[GATE].at[p // 2, two, :, :, cols]),
            )
            copies += [pltpu.make_async_copy(*pair, R["sem"].at[w, p, h]) for w, pair in enumerate(pairs)]
    for c in copies:
        c.start()
    for w in WEIGHTS:

        rows = R["mb", w].shape[0]

        def gather(i, w=w, rows=rows):
            for n in "mv":
                for h in BOTH:
                    R[n + "b", w][i, h : h + 1] = R[n + "o", w][pl.ds(rows * h + i, 1), :]

        fori(rows, gather)
        for i, n in enumerate("mv"):
            copies.append(pltpu.make_async_copy(R[n + "b", w], R[n + "out", w], R["small"].at[i, w]))
            copies[-1].start()
    for c in copies:
        c.wait()


def call(kernel, ins, outs, scratch, place_in, place_out, **params):
    names = (*ins, *outs, *scratch)
    got = pl.pallas_call(
        lambda *refs: kernel(names, *refs),
        out_shape=list(outs.values()),
        in_specs=[pl.BlockSpec(memory_space=place_in)] * len(ins),
        out_specs=[pl.BlockSpec(memory_space=place_out)] * len(outs),
        scratch_shapes=list(scratch.values()),
        name=kernel.__name__,
        compiler_params=pltpu.CompilerParams(**params),
    )(*ins.values())
    return dict(zip(outs, got, strict=True))


def by_weight(**of):
    return {(n, w): t for n, ts in of.items() for w, t in zip(WEIGHTS, ts)}


def solution(mesh):
    def step(*arrays):
        terms, weights, m, v = ([arrays[i + j] for j in (1, 2, 0)] for i in (0, 3, 6, 9))
        (rows, ff), (rows_d, d) = m[0].shape[1:], m[1].shape[1:]
        half, n, n_d = ff // 2, N * rows, N * rows_d
        full = ((2, N, N, n, ff), (2, N, N, n_d, d), (2, N, N, n, ff))
        g = [t.reshape(s) for t, s in zip(terms, (*full[:2], (2, N, 2, 2 * n, ff)))]
        state = [[pltpu.with_memory_space_constraint(a.transpose(1, 0, 2), pltpu.HBM) for a in t] for t in (m, v)]
        weights = [a.reshape(s) for a, s in zip(weights, full)]
        ins = by_weight(g=g, wt=weights, mi=state[0], vi=state[1])

        vm, dma = pltpu.VMEM, pltpu.SemaphoreType.DMA
        pad = TILE
        chunk = ((n, ff), (2, n_d, d // 2), (2 * n, half))
        own = ((2 * rows, ff), (2 * rows_d, d), (2 * rows, ff))
        down = (2 * rows_d, d // 2)
        pieces = [vm((N, *s), F32) for s in (own[0], down, (pad, half))]
        scratch = by_weight(
            own1=[vm((2, N, *c), BF) for c in chunk],
            own2=[vm((2, N, *c), BF) for c in chunk],
            r=[vm((3, 2, N, *c), BF) for c in chunk],
            ws=[vm(s, F32) for s in own],
            ms=[vm(s, F32) for s in own],
            vs=[vm(s, F32) for s in own],
            pieces=pieces,
            wl=[vm((2, n, ff), BF), vm((2, n_d, d), BF)],
            mv=[vm((2, *a.shape), F32) for a in state[0][:2]],
            tall=[vm((n, ff), F32), vm((n_d, d // 2), F32)],
        )
        scratch |= {("qa", w): vm((2, 3, *chunk[w]), BF) for w in (UP, GATE)}
        scratch |= dict(
            pb=vm((2, N, *down), F32),
            bs=vm((2, N, 3, *down), BF),
            qb=vm((2, N, 3, *down), BF),
            bt=vm((2, 3, *down), BF),
            rb=vm((2, 3, *down), BF),
            fa=vm(own[0], F32),
            sa=vm((N, *own[0]), BF),
            ra=vm((3, *own[0]), BF),
            fc=vm((N, n, half), F32),
            sc=vm((N, n, half), BF),
            rc=vm((3, n, half), BF),
            tsc=vm((N, pad, half), BF),
            tc=vm((N, pad, half), BF),
            ub=vm((N, N, *own[1]), BF),
            uc=vm((N, pad, half), BF),
            vc=vm((N, pad, half), BF),
            nsend=vm((1, 128), F32),
            nrecv=vm((N**3, 1, 128), F32),
            sent=dma((24,)),
            local=dma((N, 3, 2)),
            rec1=dma((3, 3, 2, N)),
            rec2=dma((2, 2, 3)),
            rec2b=dma((2, N, 3)),
            rec3=dma((N, 3)),
            recn=dma((1,)),
            rech=dma((N + 2, N)),
        )
        outs = by_weight(
            W=[jax.ShapeDtypeStruct(s, BF) for s in ((N, N, 2, n, ff), (N, N, 2, n_d, d), (N, N, N, n, half))],
            mo=[jax.ShapeDtypeStruct(s, F32) for s in own],
            vo=[jax.ShapeDtypeStruct(s, F32) for s in own],
        )
        count = float(N**3 * sum(a.size for a in m))

        def main(names, *refs):
            main_kernel(names, count, *refs)

        got = call(main, ins, outs, scratch, pltpu.HBM, vm, collective_id=0, has_side_effects=True, vmem_limit_bytes=36900000)
        small = [jax.ShapeDtypeStruct(a.shape, F32) for a in state[0]]
        outs = by_weight(out=[jax.ShapeDtypeStruct(s, BF) for s in full], mout=small, vout=small)
        scratch = by_weight(mb=[vm(a.shape, F32) for a in small], vb=[vm(a.shape, F32) for a in small])
        scratch |= dict(sem=dma((3, N, 2)), small=dma((2, 3)))
        new = call(write_kernel, got, outs, scratch, vm, pltpu.HBM, vmem_limit_bytes=2000000)
        back = (GATE, UP, DOWN)
        whole = [new["out", w].reshape(2, -1, full[w][-1]) for w in back]
        return (*whole, *(new[n, w].transpose(1, 0, 2) for n in ("mout", "vout") for w in back))

    all_of, part = P(None, None, None), P(None, "dp", None)
    return jax.shard_map(
        step,
        mesh=mesh,
        in_specs=(P(("rep", "dp"), None, None, None),) * 3 + (all_of,) * 3 + (part,) * 6,
        out_specs=(P("rep", None, None),) * 3 + (P("rep", "dp", None),) * 6,
        check_vma=False,
    )
```

```python
import jax
import jax.numpy as jnp
from jax import lax
from jax.experimental import pallas as pl
from jax.experimental.pallas import tpu as pltpu
from jax.sharding import PartitionSpec as P

UP, DOWN, GATE = WEIGHTS = range(3)
N = 4
QUARTERS = range(N)
FLOWS = BOTH = range(2)
ALL = [(w, h) for h in FLOWS for w in WEIGHTS]
STRIDE = {"x": N * N, "y": N, "z": 1}
AXES = (("x", "y", "z"), ("y", "z", "x"), ("z", "x", "y"))
CHUNK_AXIS = ("y", "x", "x")
FAR_FIRST = (2, 1, 3)
OUTWARD = (0, -1, 1, 2)
NEAR = (-1, 1)
TILE = 16
BF, F32 = jnp.bfloat16, jnp.float32


def fori(n, body):
    lax.fori_loop(0, n, lambda i, c: (body(i), c)[1], 0)


def main_kernel(names, count, *refs):
    R = dict(zip(names, refs, strict=True))

    def three(name):
        return [R[name, w] for w in WEIGHTS]

    g, wt, mi, vi, W, mo, vo = (three(n) for n in ("g", "wt", "mi", "vi", "W", "mo", "vo"))
    own1, own2, r, ws, ms, vs, pieces = (three(n) for n in ("own1", "own2", "r", "ws", "ms", "vs", "pieces"))
    wl, mv = ([R[n, UP], R[n, DOWN], R[n, UP]] for n in ("wl", "mv"))
    tall = [R["tall", UP], R["tall", DOWN], R["tall", UP]]
    qa = {w: R["qa", w] for w in (UP, GATE)}
    gf = mo
    pb, bs, qb, bt, rb, fa, sa, ra, fc, sc, rc, tsc, tc, ub, uc, vc, nsend, nrecv = (
        R[n] for n in ("pb", "bs", "qb", "bt", "rb", "fa", "sa", "ra", "fc", "sc", "rc", "tsc", "tc", "ub", "uc", "vc", "nsend", "nrecv")
    )
    ua = sa
    sent, local, rec1, recd, rec2, rec2b, rec3, recn, rech = (
        R[n] for n in ("sent", "local", "rec1", "recd", "rec2", "rec2b", "rec3", "recn", "rech")
    )
    tokens = iter(range(sent.shape[0]))
    leaving = []

    me = lax.axis_index("dp")
    co = {"x": me // STRIDE["x"], "y": me // STRIDE["y"] % N, "z": me % N}
    x, y, z = co["x"], co["y"], co["z"]

    def at(axis, off):
        return (co[axis] + off) % N

    def to(axis, off):
        return me + (at(axis, off) - co[axis]) * STRIDE[axis]

    def group(ref):
        sem = sent.at[next(tokens)]
        leaving.append((ref, sem))
        return sem

    def post(src, dst, ssem, rsem, device):
        pltpu.make_async_remote_copy(
            src_ref=src, dst_ref=dst, send_sem=ssem, recv_sem=rsem, device_id={"dp": device}, device_id_type=pl.DeviceIdType.MESH
        ).start()

    def send(src, dst, ssem, rsem, axis, off):
        post(src, dst, ssem, rsem, to(axis, off))

    def wait(ref, sem):
        pltpu.make_async_copy(ref, ref, sem).wait()

    def way(h):
        return 1 - 2 * h

    def offs(w, h):
        return (2, 1, -1, 0) if w == DOWN else (2, -way(h), way(h), 0)

    def term(w, h, q, c):
        if w == UP:
            return g[w].at[h, q, c]
        if w == DOWN:
            return g[w].at[:, c, q, :, down_cols(h)]
        cols = g[w].shape[-1] // 2
        return g[w].at[q // 2, c, h, :, pl.ds(pl.multiple_of(q % 2 * cols, 128), cols)]

    def rows_of(i):
        return pl.ds(pl.multiple_of(i * TILE, TILE), TILE)

    def tiles(w, body):
        n = own1[w].shape[-2] // TILE
        if w == DOWN:
            fori(2 * n, lambda i: body((i // n, rows_of(i % n))))
        else:
            fori(n, lambda i: body((rows_of(i),)))

    def parts(w):
        cols = own1[w].shape[-1]
        cut_at = (cols // 128 + 1) // 2 * 128
        return slice(0, cut_at), slice(cut_at, cols)

    def down_cols(h):
        cols = own1[DOWN].shape[-1]
        return pl.ds(h * cols, cols)

    def cut(w, h, part=slice(None)):
        rows, cols = vi[w].shape[0], pieces[w].shape[-1]
        for q in QUARTERS:
            pieces[w][q, rows * h : rows * (h + 1), part] = tall[w][rows * q : rows * (q + 1), 0:cols][:, part]

    def join(w, h):
        rows, cols = vi[w].shape[0], pieces[w].shape[-1]
        for q in QUARTERS:
            tall[w][rows * q : rows * (q + 1), 0:cols] = pieces[w][q, rows * h : rows * (h + 1)]
        return tall[w][0 : N * rows, 0:cols].astype(BF)

    barrier = pltpu.get_barrier_semaphore()
    for axis in STRIDE:
        for off in NEAR:
            pl.semaphore_signal(barrier, inc=1, device_id={"dp": to(axis, off)}, device_id_type=pl.DeviceIdType.MESH)

    early = three("early")

    def first_term(w, h):
        return term(w, h, at(AXES[w][0], 2), at(CHUNK_AXIS[w], offs(w, h)[0]))

    for w, h in ALL:
        pltpu.make_async_copy(first_term(w, h), early[w].at[h], local.at[5, w]).start()
    for which, buf in enumerate((own1, own2)):
        for w, h in ALL:
            q = at(AXES[w][0], way(h) * (1 - which))
            for k in QUARTERS:
                src = term(w, h, q, at(CHUNK_AXIS[w], offs(w, h)[k]))
                pltpu.make_async_copy(src, buf[w].at[h, k], local.at[which, w]).start()
    pl.semaphore_wait(barrier, len(STRIDE) * len(NEAR))

    for w in WEIGHTS:
        wait(early[w], local.at[5, w])
    left1 = [group(r[w]) for w in WEIGHTS]

    def phase1(i, w, h, k, src, off):
        sem = recd.at[w, h] if i == 1 else rec1.at[w, i // 2, h, k]
        send(src, r[w].at[i, h, k], left1[w], sem, AXES[w][0], off)

    for i, (far, near) in enumerate(((2, 1), (-1, -1))):
        for k in QUARTERS:
            for w, h in ALL:
                s = way(h)
                src = early[w].at[h]
                if i or k:
                    src = term(w, h, at(AXES[w][0], far * s), at(CHUNK_AXIS[w], offs(w, h)[k]))
                phase1(i, w, h, k, src, near * s)

    def load_state(w):
        for i, (src, dst) in enumerate(((wt[w].at[:, x, y], wl[w]), (mi[w], mv[w].at[0]), (vi[w], mv[w].at[1]))):
            pltpu.make_async_copy(src, dst, local.at[2 + i, w]).start()

    load_state(UP)
    load_state(DOWN)
    for which, buf in enumerate((own1, own2)):
        for w in WEIGHTS:
            wait(buf[w], local.at[which, w])

    for k in QUARTERS:
        for w, h in ALL:
            wait(r[w].at[0, h, k], rec1.at[w, 0, h, k])

            def add(t, w=w, h=h, k=k):
                t = (h, k, *t)
                own1[w][t] = (own1[w][t].astype(F32) + r[w][(0, *t)].astype(F32)).astype(BF)

            tiles(w, add)
            phase1(2, w, h, k, own1[w].at[h, k], way(h))

    pieces[GATE][...] = jnp.zeros(pieces[GATE].shape, F32)
    for w in WEIGHTS:
        rows = vi[w].shape[0]
        for i, dst in enumerate((wl[w], mv[w].at[0], mv[w].at[1])):
            wait(dst, local.at[2 + i, w])

        def spread(i, w=w, rows=rows):
            for src, dst in ((mv[w][0, i], ms[w]), (mv[w][1, i], vs[w])):
                for h in BOTH:
                    dst[pl.ds(rows * h + i, 1), :] = src[h : h + 1]

        fori(rows, spread)
        v = DOWN if w == DOWN else UP
        for cols in [down_cols(c) for c in BOTH] if w == DOWN else [slice(None)]:
            for h in BOTH:

                def widen(i, w=w, h=h, v=v, cols=cols):
                    t = rows_of(i)
                    tall[v][t, :] = wl[w][h, t, cols].astype(F32)

                fori(N * rows // TILE, widen)
                cut(v, h)
            ws[w][:, cols] = pieces[v][z]
        if w == UP:
            load_state(GATE)

    def total(w, h, k, t):
        t = (h, k, *t)
        return own2[w][t].astype(F32) + r[w][(1, *t)].astype(F32) + r[w][(2, *t)].astype(F32)

    def cut_down(h, k):
        n = own2[DOWN].shape[-2]
        for layer in BOTH:

            def put(i, layer=layer):
                t = rows_of(i)
                tall[DOWN][t, :] = total(DOWN, h, k, (layer, t))

            fori(n // TILE, put)
            cut(DOWN, layer)

    left2 = {w: group(qa[w]) for w in qa}
    left2b = group(qb)

    def phase2(i, w, h, off, part=None):
        for p in BOTH if part is None else (part,):
            cols = (slice(None), parts(w)[p])
            src, dst = own2[w].at[h, i], qa[w].at[h, i]
            send(src.at[cols], dst.at[cols], left2[w], rec2.at[w // 2, h, p, min(i, 1)], AXES[w][1], off)

    def phase2b(i, h, k, off):
        send(bs.at[h, k, i], qb.at[h, k, i], left2b, rec2b.at[h, k, min(i, 1)], "z", off)

    for k in QUARTERS:
        for w, h in ALL:
            s = way(h)
            if not k:
                wait(r[w].at[1, h], recd.at[w, h])
            wait(r[w].at[2, h, k], rec1.at[w, 1, h, k])
            if w == DOWN:
                cut_down(h, k)
                pb[h, k] = pieces[w][z]
                for i, (far, near) in enumerate(((2, 1), (-1, -1))):
                    bs[h, k, i] = pieces[w][at("z", far * s)].astype(BF)
                    phase2b(i, h, k, near * s)
            elif k < 2:

                def put(t, w=w, h=h, k=k):
                    own2[w][(h, k, *t)] = total(w, h, k, t).astype(BF)

                tiles(w, put)
                phase2(k, w, h, -s if k else s)

    def running(p):
        for w in qa:
            cols = parts(w)[p]
            for h in FLOWS:
                wait(qa[w].at[h, 0, :, cols], rec2.at[w // 2, h, p, 0])

                def add2(t, w=w, h=h, cols=cols):
                    t = (*t, cols)
                    own2[w][(h, 2, *t)] = (total(w, h, 2, t) + qa[w][(h, 0, *t)].astype(F32)).astype(BF)

                tiles(w, add2)
                phase2(2, w, h, way(h), p)

    def running_down(k):
        for h in FLOWS:
            s = way(h)
            cut_down(h, k)
            wait(qb.at[h, k, 0], rec2b.at[h, k, 0])
            bs[h, k, 2] = (pieces[DOWN][at("z", s)] + qb[h, k, 0].astype(F32)).astype(BF)
            phase2b(2, h, k, s)

    left_a, left_c, left_b = group(ra), group(rc), group(rb)

    def last_sends(p):
        for w in qa:
            cols = parts(w)[p]
            for h in BOTH:
                wait(qa[w].at[h, 1:3, :, cols], rec2.at[w // 2, h, p, 1])

                def total2(t, w=w, h=h, cols=cols):
                    t = (*t, cols)
                    return total(w, h, 3, t) + qa[w][(h, 1, *t)].astype(F32) + qa[w][(h, 2, *t)].astype(F32)

                if w == UP:

                    def put2(t, total2=total2, cols=cols):
                        tall[UP][(*t, cols)] = total2(t)

                    tiles(w, put2)
                    cut(UP, h, cols)
                else:
                    n = fc.shape[1]
                    for b in BOTH:

                        def put2(i, total2=total2, h=h, b=b, n=n, cols=cols):
                            v = total2((pl.ds(pl.multiple_of(b * n + i * TILE, TILE), TILE),))
                            t = rows_of(i)
                            fc[2 * h + b, t, cols] = v
                            sc[2 * h + b, t, cols] = v.astype(BF)

                        fori(n // TILE, put2)
            if w == UP:
                for q in QUARTERS:
                    sa[q, :, cols] = pieces[UP][q, :, cols].astype(BF)
                fa[:, cols] = pieces[UP][z, :, cols]
            for j in FAR_FIRST:
                src, dst, left, axis = (sa, ra, left_a, "z") if w == UP else (sc, rc, left_c, "y")
                send(src.at[at(axis, j), :, cols], dst.at[j - 1, :, cols], left, rec3.at[w // 2, p], axis, j)

    def last_sends_down(k):
        for h in BOTH:
            wait(qb.at[h, k, 1:3], rec2b.at[h, k, 1])
            v = pb[h, k] + qb[h, k, 1].astype(F32) + qb[h, k, 2].astype(F32)
            off = offs(DOWN, h)[k]
            if off:
                bt[h, k] = v.astype(BF)
                send(bt.at[h, k], rb.at[h, k], left_b, rec3.at[2, h], "x", off)
            else:
                pb[h, k] = v

    first, second = BOTH
    running(first)
    running_down(0)
    running_down(1)
    running(second)
    running_down(2)
    running_down(3)
    last_sends(first)
    last_sends_down(0)
    last_sends_down(1)
    last_sends(second)
    last_sends_down(2)
    last_sends_down(3)

    def fold(v):
        v = jnp.sum(v * v, axis=0, keepdims=True)
        out = v[:, 0:128]
        for i in range(128, v.shape[1], 128):
            out = out + v[:, i : i + 128]
        nsend[...] = nsend[...] + out

    def rounded(own, others):
        for o in others:
            own = own + o.astype(F32)
        return own.astype(BF).astype(F32)

    others = range(len(FAR_FIRST))
    half = tsc.shape[-1]
    nsend[...] = jnp.zeros(nsend.shape, F32)
    for p in BOTH:
        wait(rc.at[:, :, parts(GATE)[p]], rec3.at[1, p])

    def last_c(i):
        t = rows_of(i)
        v = rounded(fc[y, t], [rc[j, t] for j in others])
        tall[UP][t, 0:half] = v
        fold(v)

    fori(fc.shape[1] // TILE, last_c)
    cut(GATE, 0)
    for q in QUARTERS:
        tsc[q] = pieces[GATE][q].astype(BF)
    tc[z] = tsc[z]
    left = group(tc.at[0:3])
    for j in FAR_FIRST:
        send(tsc.at[at("z", j)], tc.at[z], left, rech.at[0], "z", j)
    for p in BOTH:
        wait(ra.at[:, :, parts(UP)[p]], rec3.at[0, p])
    (gone,) = [i for i, (_, sem) in enumerate(leaving) if sem is left_a]
    wait(*leaving.pop(gone))
    v = rounded(fa[...], [ra[j] for j in others])
    gf[UP][...] = v
    fold(v)
    for h in BOTH:
        wait(rb.at[h], rec3.at[2, h])
        v = rounded(pb[h, 3], [rb[h, k] for k in others])
        gf[DOWN][:, down_cols(h)] = v
        fold(v)

    devices = nrecv.shape[0]
    nrecv[me] = nsend[...]
    left = group(nrecv.at[1:devices])
    away = [(min(i, N - i), i) for i in QUARTERS]
    for _, i, j, k in sorted((a + b + c, i, j, k) for a, i in away for b, j in away for c, k in away)[:0:-1]:
        post(nsend, nrecv.at[me], left, recn.at[0], to("x", i) + to("y", j) + to("z", k) - 2 * me)
    wait(tc.at[0:3], rech.at[0])
    wait(nrecv.at[1:devices], recn.at[0])
    squares = jnp.sum(jnp.sum(nrecv[...], axis=0), axis=1, keepdims=True)
    factor = jnp.minimum(1.0, 0.5 * lax.rsqrt(squares / count + 1e-30))
    rows = vi[GATE].shape[0]

    def gate_part(q):
        return slice(rows * (q // 2), rows * (q // 2 + 1)), slice(half * (q % 2), half * (q % 2 + 1))

    for q in QUARTERS:
        gf[GATE][gate_part(q)] = tc[q].astype(F32)[:rows]

    def adamw(w):
        gc = gf[w][...] * factor
        m = 0.9 * ms[w][...] + 0.1 * gc
        v = 0.95 * vs[w][...] + 0.05 * gc * gc
        mo[w][...] = m
        vo[w][...] = v
        step = m * lax.rsqrt(v + 1e-8) + 0.1 * ws[w][...]
        return ws[w][...] - 0.02 * step

    def spread_out(i, axis, ref, first):
        left = group(first)
        for j in FAR_FIRST:
            send(ref(co[axis]), ref(co[axis]), left, rech.at[i], axis, j)

    pieces[UP][0] = adamw(GATE)
    for q in QUARTERS:
        pieces[GATE][q, 0:rows] = pieces[UP][(0, *gate_part(q))]
        vc[q] = pieces[GATE][q].astype(BF)
    uc[z] = vc[z]
    left = group(uc.at[0:3])
    for j in FAR_FIRST:
        send(vc.at[at("z", j)], uc.at[z], left, rech.at[2], "z", j)
    ua[z] = adamw(UP).astype(BF)
    spread_out(1, "z", lambda p: ua.at[p], ua.at[0:3])
    ub[z, x] = adamw(DOWN).astype(BF)
    left = group(ub.at[0, 0:3])
    for j in FAR_FIRST:
        send(ub.at[z, x], ub.at[z, x], left, rech.at[N + j], "x", j)

    class Ring:
        def __init__(self, ref, sub, left, recv, axis):
            self.ref, self.sub, self.left, self.recv, self.axis = ref, sub, left, recv, axis

        def half(self, p, h):
            return self.ref(p).at[self.sub(h)]

        def own(self, h):
            for d in BOTH:
                ref = self.half(0, h)
                send(ref, ref, self.left, self.recv(d, h), self.axis, way(d))

        def owns(self):
            for h in BOTH:
                self.own(h)

        def pass_on(self):
            for d in BOTH:
                ref = self.half(NEAR[d], d)
                wait(ref, self.recv(d, d))
                send(ref, ref, self.left, self.recv(2, d), self.axis, way(d))

        def near(self, d):
            wait(self.half(NEAR[d], 1 - d), self.recv(d, 1 - d))

        def far(self):
            for d in BOTH:
                wait(self.half(2, d), self.recv(2, d))

    def one(h):
        return h

    def two(h):
        return pl.ds(2 * h, 2)

    def outer_ring(w, i, left):
        a, c = AXES[w][0], CHUNK_AXIS[w]
        return Ring(
            lambda p: W[w].at[at(a, p), at(c, OUTWARD[i])],
            two if w == GATE else one,
            left,
            lambda u, v: rec1.at[w, 0, u, i] if u == v else recd.at[w, u // 2],
            a,
        )

    left_o = [group(W[w].at[0:3]) for w in WEIGHTS]
    outer = [[outer_ring(w, i, left_o[w]) for i in QUARTERS] for w in WEIGHTS]
    left_z, left_y, left_x = group(ub.at[0:3]), group(W[UP].at[0, 0:3]), group(W[GATE].at[0, 0:3])
    zring = [
        Ring(lambda p, off=off: ub.at[at("z", p), at("x", off)], lambda h: (slice(None), down_cols(h)), left_z, lambda u, v, i=i: rec2b.at[u, i, 0] if u == v else rec2b.at[0, i, 1], "z")
        for i, off in enumerate(OUTWARD)
    ]
    yring = Ring(lambda p: W[UP].at[x, at("y", p)], one, left_y, lambda u, v: rec2.at[0, v, u % 2, u // 2], "y")
    xring = Ring(lambda p: W[GATE].at[z, at("x", p)], two, left_x, lambda u, v: rec2.at[1, v, u % 2, u // 2], "x")

    zring[0].owns()
    wait(uc.at[0:3], rech.at[2])
    for q in QUARTERS:
        pieces[GATE][q] = uc[q].astype(F32)
    W[GATE][z, x, y] = join(GATE, 0)
    spread_out(3, "y", lambda p: W[GATE].at[z, x, p], W[GATE].at[0, 0, 0:3])
    for i, off in enumerate(OUTWARD):
        if off:
            wait(ub.at[z, at("x", off)], rech.at[N - off % N + N])
            zring[i].owns()
    wait(ua.at[0:3], rech.at[1])
    for q in QUARTERS:
        pieces[UP][q] = ua[q].astype(F32)
    for h in BOTH:
        W[UP][x, y, h] = join(UP, h)
        yring.own(h)
        outer[UP][0].own(h)
    zring[0].pass_on()
    wait(W[GATE].at[0, 0, 0:3], rech.at[3])
    xring.owns()
    for i in QUARTERS:
        if i:
            zring[i].pass_on()
    outer[GATE][0].owns()
    yring.pass_on()
    for d in BOTH:
        yring.near(d)
    outer[UP][1].owns()
    for i in QUARTERS:
        wait(ub.at[0:2, 0], rec2b.at[0, i, 1])
        c = at("x", OUTWARD[i])
        for d in BOTH:
            for q in QUARTERS:
                pieces[DOWN][q] = ub[q, c, :, down_cols(d)].astype(F32)
            for h in BOTH:
                W[DOWN][y, c, h, :, down_cols(d)] = join(DOWN, h)
        outer[DOWN][i].owns()
    xring.pass_on()
    for d in BOTH:
        xring.near(d)
    outer[UP][2].owns()
    outer[GATE][1].owns()
    outer[GATE][2].owns()
    yring.far()
    outer[UP][3].owns()
    xring.far()
    outer[GATE][3].owns()
    for i in QUARTERS:
        for w in WEIGHTS:
            outer[w][i].pass_on()
    for w in WEIGHTS:
        for i in BOTH:
            wait(W[w].at[0], recd.at[w, i])
    for ref, sem in leaving:
        wait(ref, sem)


def write_kernel(names, *refs):
    R = dict(zip(names, refs, strict=True))
    W = [R["W", w] for w in WEIGHTS]
    out = [R["out", w] for w in WEIGHTS]
    half = W[GATE].shape[-1]
    copies = []
    for p in QUARTERS:
        for h in BOTH:
            cols, two = pl.ds(half * (p % 2), half), pl.ds(2 * h, 2)
            pairs = (
                (W[UP].at[p, :, h], out[UP].at[h, p]),
                (W[DOWN].at[p, :, h], out[DOWN].at[h, :, p]),
                (W[GATE].at[p, two], out[GATE].at[p // 2, two, :, :, cols]),
            )
            copies += [pltpu.make_async_copy(*pair, R["sem"].at[w, p, h]) for w, pair in enumerate(pairs)]
    for c in copies:
        c.start()
    for w in WEIGHTS:

        rows = R["mb", w].shape[0]

        def gather(i, w=w, rows=rows):
            for n in "mv":
                for h in BOTH:
                    R[n + "b", w][i, h : h + 1] = R[n + "o", w][pl.ds(rows * h + i, 1), :]

        fori(rows, gather)
        for i, n in enumerate("mv"):
            copies.append(pltpu.make_async_copy(R[n + "b", w], R[n + "out", w], R["small"].at[i, w]))
            copies[-1].start()
    for c in copies:
        c.wait()


def call(kernel, ins, outs, scratch, place_in, place_out, **params):
    names = (*ins, *outs, *scratch)
    got = pl.pallas_call(
        lambda *refs: kernel(names, *refs),
        out_shape=list(outs.values()),
        in_specs=[pl.BlockSpec(memory_space=place_in)] * len(ins),
        out_specs=[pl.BlockSpec(memory_space=place_out)] * len(outs),
        scratch_shapes=list(scratch.values()),
        name=kernel.__name__,
        compiler_params=pltpu.CompilerParams(**params),
    )(*ins.values())
    return dict(zip(outs, got, strict=True))


def by_weight(**of):
    return {(n, w): t for n, ts in of.items() for w, t in zip(WEIGHTS, ts)}


def solution(mesh):
    def step(*arrays):
        terms, weights, m, v = ([arrays[i + j] for j in (1, 2, 0)] for i in (0, 3, 6, 9))
        (rows, ff), (rows_d, d) = m[0].shape[1:], m[1].shape[1:]
        half, n, n_d = ff // 2, N * rows, N * rows_d
        full = ((2, N, N, n, ff), (2, N, N, n_d, d), (2, N, N, n, ff))
        g = [t.reshape(s) for t, s in zip(terms, (*full[:2], (2, N, 2, 2 * n, ff)))]
        state = [[pltpu.with_memory_space_constraint(a.transpose(1, 0, 2), pltpu.HBM) for a in t] for t in (m, v)]
        weights = [a.reshape(s) for a, s in zip(weights, full)]
        ins = by_weight(g=g, wt=weights, mi=state[0], vi=state[1])

        vm, dma = pltpu.VMEM, pltpu.SemaphoreType.DMA
        pad = TILE
        chunk = ((n, ff), (2, n_d, d // 2), (2 * n, half))
        own = ((2 * rows, ff), (2 * rows_d, d), (2 * rows, ff))
        down = (2 * rows_d, d // 2)
        pieces = [vm((N, *s), F32) for s in (own[0], down, (pad, half))]
        scratch = by_weight(
            own1=[vm((2, N, *c), BF) for c in chunk],
            own2=[vm((2, N, *c), BF) for c in chunk],
            early=[vm((2, *c), BF) for c in chunk],
            r=[vm((3, 2, N, *c), BF) for c in chunk],
            ws=[vm(s, F32) for s in own],
            ms=[vm(s, F32) for s in own],
            vs=[vm(s, F32) for s in own],
            pieces=pieces,
            wl=[vm((2, n, ff), BF), vm((2, n_d, d), BF)],
            mv=[vm((2, *a.shape), F32) for a in state[0][:2]],
            tall=[vm((n, ff), F32), vm((n_d, d // 2), F32)],
        )
        scratch |= {("qa", w): vm((2, 3, *chunk[w]), BF) for w in (UP, GATE)}
        scratch |= dict(
            pb=vm((2, N, *down), F32),
            bs=vm((2, N, 3, *down), BF),
            qb=vm((2, N, 3, *down), BF),
            bt=vm((2, 3, *down), BF),
            rb=vm((2, 3, *down), BF),
            fa=vm(own[0], F32),
            sa=vm((N, *own[0]), BF),
            ra=vm((3, *own[0]), BF),
            fc=vm((N, n, half), F32),
            sc=vm((N, n, half), BF),
            rc=vm((3, n, half), BF),
            tsc=vm((N, pad, half), BF),
            tc=vm((N, pad, half), BF),
            ub=vm((N, N, *own[1]), BF),
            uc=vm((N, pad, half), BF),
            vc=vm((N, pad, half), BF),
            nsend=vm((1, 128), F32),
            nrecv=vm((N**3, 1, 128), F32),
            sent=dma((24,)),
            local=dma((6, 3)),
            rec1=dma((3, 2, 2, N)),
            recd=dma((3, 2)),
            rec2=dma((2, 2, 2, 2)),
            rec2b=dma((2, N, 2)),
            rec3=dma((3, 2)),
            recn=dma((1,)),
            rech=dma((2 * N,)),
        )
        outs = by_weight(
            W=[jax.ShapeDtypeStruct(s, BF) for s in ((N, N, 2, n, ff), (N, N, 2, n_d, d), (N, N, N, n, half))],
            mo=[jax.ShapeDtypeStruct(s, F32) for s in own],
            vo=[jax.ShapeDtypeStruct(s, F32) for s in own],
        )
        count = float(N**3 * sum(a.size for a in m))

        def main(names, *refs):
            main_kernel(names, count, *refs)

        got = call(main, ins, outs, scratch, pltpu.HBM, vm, collective_id=0, has_side_effects=True, vmem_limit_bytes=37600000)
        small = [jax.ShapeDtypeStruct(a.shape, F32) for a in state[0]]
        outs = by_weight(out=[jax.ShapeDtypeStruct(s, BF) for s in full], mout=small, vout=small)
        scratch = by_weight(mb=[vm(a.shape, F32) for a in small], vb=[vm(a.shape, F32) for a in small])
        scratch |= dict(sem=dma((3, N, 2)), small=dma((2, 3)))
        new = call(write_kernel, got, outs, scratch, vm, pltpu.HBM, vmem_limit_bytes=2000000)
        back = (GATE, UP, DOWN)
        whole = [new["out", w].reshape(2, -1, full[w][-1]) for w in back]
        return (*whole, *(new[n, w].transpose(1, 0, 2) for n in ("mout", "vout") for w in back))

    all_of, part = P(None, None, None), P(None, "dp", None)
    return jax.shard_map(
        step,
        mesh=mesh,
        in_specs=(P(("rep", "dp"), None, None, None),) * 3 + (all_of,) * 3 + (part,) * 6,
        out_specs=(P("rep", None, None),) * 3 + (P("rep", "dp", None),) * 6,
        check_vma=False,
    )
```

```python
import jax
import jax.numpy as jnp
from jax import lax
from jax.experimental import pallas as pl
from jax.experimental.pallas import tpu as pltpu
from jax.sharding import PartitionSpec as P

UP, DOWN, GATE = WEIGHTS = range(3)
N = 4
QUARTERS = range(N)
FLOWS = BOTH = range(2)
ALL = [(w, h) for h in FLOWS for w in WEIGHTS]
STRIDE = {"x": N * N, "y": N, "z": 1}
AXES = (("x", "y", "z"), ("y", "z", "x"), ("z", "x", "y"))
CHUNK_AXIS = ("y", "x", "x")
FAR_FIRST = (2, 1, 3)
OUTWARD = (0, -1, 1, 2)
NEAR = (-1, 1)
TILE = 16
BF, F32 = jnp.bfloat16, jnp.float32


def fori(n, body):
    lax.fori_loop(0, n, lambda i, c: (body(i), c)[1], 0)


def main_kernel(names, count, *refs):
    R = dict(zip(names, refs, strict=True))

    def three(name):
        return [R[name, w] for w in WEIGHTS]

    g, wt, mi, vi, W, mo, vo = (three(n) for n in ("g", "wt", "mi", "vi", "W", "mo", "vo"))
    own1, own2, r, ws, ms, vs, pieces = (three(n) for n in ("own1", "own2", "r", "ws", "ms", "vs", "pieces"))
    wl, mv = ([R[n, UP], R[n, DOWN], R[n, UP]] for n in ("wl", "mv"))
    tall = [R["tall", UP], R["tall", DOWN], R["tall", UP]]
    qa = {w: R["qa", w] for w in (UP, GATE)}
    gf = mo
    pb, bs, qb, bt, rb, fa, sa, ra, fc, sc, rc, tsc, tc, ub, uc, vc, nsend, nrecv = (
        R[n] for n in ("pb", "bs", "qb", "bt", "rb", "fa", "sa", "ra", "fc", "sc", "rc", "tsc", "tc", "ub", "uc", "vc", "nsend", "nrecv")
    )
    ua = sa
    sent, local, rec1, recd, rec2, rec2b, rec3, recn, rech = (
        R[n] for n in ("sent", "local", "rec1", "recd", "rec2", "rec2b", "rec3", "recn", "rech")
    )
    tokens = iter(range(sent.shape[0]))
    leaving = []

    me = lax.axis_index("dp")
    co = {"x": me // STRIDE["x"], "y": me // STRIDE["y"] % N, "z": me % N}
    x, y, z = co["x"], co["y"], co["z"]

    def at(axis, off):
        return (co[axis] + off) % N

    def to(axis, off):
        return me + (at(axis, off) - co[axis]) * STRIDE[axis]

    def group(ref):
        sem = sent.at[next(tokens)]
        leaving.append((ref, sem))
        return sem

    def post(src, dst, ssem, rsem, device):
        pltpu.make_async_remote_copy(
            src_ref=src, dst_ref=dst, send_sem=ssem, recv_sem=rsem, device_id={"dp": device}, device_id_type=pl.DeviceIdType.MESH
        ).start()

    def send(src, dst, ssem, rsem, axis, off):
        post(src, dst, ssem, rsem, to(axis, off))

    def wait(ref, sem):
        pltpu.make_async_copy(ref, ref, sem).wait()

    def way(h):
        return 1 - 2 * h

    def offs(w, h):
        return (2, 1, -1, 0) if w == DOWN else (2, -way(h), way(h), 0)

    def term(w, h, q, c):
        if w == UP:
            return g[w].at[h, q, c]
        if w == DOWN:
            return g[w].at[:, c, q, :, down_cols(h)]
        cols = g[w].shape[-1] // 2
        return g[w].at[q // 2, c, h, :, pl.ds(pl.multiple_of(q % 2 * cols, 128), cols)]

    def rows_of(i):
        return pl.ds(pl.multiple_of(i * TILE, TILE), TILE)

    def tiles(w, body):
        n = own1[w].shape[-2] // TILE
        if w == DOWN:
            fori(2 * n, lambda i: body((i // n, rows_of(i % n))))
        else:
            fori(n, lambda i: body((rows_of(i),)))

    def parts(w):
        cols = own1[w].shape[-1]
        cut_at = (cols // 128 * 2 + 1) // 3 * 128
        return slice(0, cut_at), slice(cut_at, cols)

    def down_cols(h):
        cols = own1[DOWN].shape[-1]
        return pl.ds(h * cols, cols)

    def cut(w, h, part=slice(None)):
        rows, cols = vi[w].shape[0], pieces[w].shape[-1]
        for q in QUARTERS:
            pieces[w][q, rows * h : rows * (h + 1), part] = tall[w][rows * q : rows * (q + 1), 0:cols][:, part]

    def join(w, h):
        rows, cols = vi[w].shape[0], pieces[w].shape[-1]
        for q in QUARTERS:
            tall[w][rows * q : rows * (q + 1), 0:cols] = pieces[w][q, rows * h : rows * (h + 1)]
        return tall[w][0 : N * rows, 0:cols].astype(BF)

    barrier = pltpu.get_barrier_semaphore()
    for axis in STRIDE:
        for off in NEAR:
            pl.semaphore_signal(barrier, inc=1, device_id={"dp": to(axis, off)}, device_id_type=pl.DeviceIdType.MESH)

    early = three("early")

    def first_term(w, h):
        return term(w, h, at(AXES[w][0], 2), at(CHUNK_AXIS[w], offs(w, h)[0]))

    for w, h in ALL:
        pltpu.make_async_copy(first_term(w, h), early[w].at[h], local.at[5, w]).start()
    for which, buf in enumerate((own1, own2)):
        for w, h in ALL:
            q = at(AXES[w][0], way(h) * (1 - which))
            for k in QUARTERS:
                src = term(w, h, q, at(CHUNK_AXIS[w], offs(w, h)[k]))
                pltpu.make_async_copy(src, buf[w].at[h, k], local.at[which, w]).start()
    pl.semaphore_wait(barrier, len(STRIDE) * len(NEAR))

    for w in WEIGHTS:
        wait(early[w], local.at[5, w])
    left1 = [group(r[w]) for w in WEIGHTS]

    def phase1(i, w, h, k, src, off):
        sem = recd.at[w, h] if i == 1 else rec1.at[w, i // 2, h, k]
        send(src, r[w].at[i, h, k], left1[w], sem, AXES[w][0], off)

    for i, (far, near) in enumerate(((2, 1), (-1, -1))):
        for k in QUARTERS:
            for w, h in ALL:
                s = way(h)
                src = early[w].at[h]
                if i or k:
                    src = term(w, h, at(AXES[w][0], far * s), at(CHUNK_AXIS[w], offs(w, h)[k]))
                phase1(i, w, h, k, src, near * s)

    def load_state(w):
        for i, (src, dst) in enumerate(((wt[w].at[:, x, y], wl[w]), (mi[w], mv[w].at[0]), (vi[w], mv[w].at[1]))):
            pltpu.make_async_copy(src, dst, local.at[2 + i, w]).start()

    load_state(UP)
    load_state(DOWN)
    for which, buf in enumerate((own1, own2)):
        for w in WEIGHTS:
            wait(buf[w], local.at[which, w])

    for k in QUARTERS:
        for w, h in ALL:
            wait(r[w].at[0, h, k], rec1.at[w, 0, h, k])

            def add(t, w=w, h=h, k=k):
                t = (h, k, *t)
                own1[w][t] = (own1[w][t].astype(F32) + r[w][(0, *t)].astype(F32)).astype(BF)

            tiles(w, add)
            phase1(2, w, h, k, own1[w].at[h, k], way(h))

    pieces[GATE][...] = jnp.zeros(pieces[GATE].shape, F32)
    for w in WEIGHTS:
        rows = vi[w].shape[0]
        for i, dst in enumerate((wl[w], mv[w].at[0], mv[w].at[1])):
            wait(dst, local.at[2 + i, w])

        def spread(i, w=w, rows=rows):
            for src, dst in ((mv[w][0, i], ms[w]), (mv[w][1, i], vs[w])):
                for h in BOTH:
                    dst[pl.ds(rows * h + i, 1), :] = src[h : h + 1]

        fori(rows, spread)
        v = DOWN if w == DOWN else UP
        for cols in [down_cols(c) for c in BOTH] if w == DOWN else [slice(None)]:
            for h in BOTH:

                def widen(i, w=w, h=h, v=v, cols=cols):
                    t = rows_of(i)
                    tall[v][t, :] = wl[w][h, t, cols].astype(F32)

                fori(N * rows // TILE, widen)
                cut(v, h)
            ws[w][:, cols] = pieces[v][z]
        if w == UP:
            load_state(GATE)

    def total(w, h, k, t):
        t = (h, k, *t)
        return own2[w][t].astype(F32) + r[w][(1, *t)].astype(F32) + r[w][(2, *t)].astype(F32)

    def cut_down(h, k):
        n = own2[DOWN].shape[-2]
        for layer in BOTH:

            def put(i, layer=layer):
                t = rows_of(i)
                tall[DOWN][t, :] = total(DOWN, h, k, (layer, t))

            fori(n // TILE, put)
            cut(DOWN, layer)

    left2 = {w: group(qa[w]) for w in qa}
    left2b = group(qb)

    def phase2(i, w, h, off, part=None):
        for p in BOTH if part is None else (part,):
            cols = (slice(None), parts(w)[p])
            src, dst = own2[w].at[h, i], qa[w].at[h, i]
            send(src.at[cols], dst.at[cols], left2[w], rec2.at[w // 2, h, p, min(i, 1)], AXES[w][1], off)

    def phase2b(i, h, k, off):
        send(bs.at[h, k, i], qb.at[h, k, i], left2b, rec2b.at[h, k, min(i, 1)], "z", off)

    for k in QUARTERS:
        for w, h in ALL:
            s = way(h)
            if not k:
                wait(r[w].at[1, h], recd.at[w, h])
            wait(r[w].at[2, h, k], rec1.at[w, 1, h, k])
            if w == DOWN:
                cut_down(h, k)
                pb[h, k] = pieces[w][z]
                for i, (far, near) in enumerate(((2, 1), (-1, -1))):
                    bs[h, k, i] = pieces[w][at("z", far * s)].astype(BF)
                    phase2b(i, h, k, near * s)
            elif k < 2:

                def put(t, w=w, h=h, k=k):
                    own2[w][(h, k, *t)] = total(w, h, k, t).astype(BF)

                tiles(w, put)
                phase2(k, w, h, -s if k else s)

    def running(p):
        for w in qa:
            cols = parts(w)[p]
            for h in FLOWS:
                wait(qa[w].at[h, 0, :, cols], rec2.at[w // 2, h, p, 0])

                def add2(t, w=w, h=h, cols=cols):
                    t = (*t, cols)
                    own2[w][(h, 2, *t)] = (total(w, h, 2, t) + qa[w][(h, 0, *t)].astype(F32)).astype(BF)

                tiles(w, add2)
                phase2(2, w, h, way(h), p)

    def running_down(k):
        for h in FLOWS:
            s = way(h)
            cut_down(h, k)
            wait(qb.at[h, k, 0], rec2b.at[h, k, 0])
            bs[h, k, 2] = (pieces[DOWN][at("z", s)] + qb[h, k, 0].astype(F32)).astype(BF)
            phase2b(2, h, k, s)

    left_a, left_c, left_b = group(ra), group(rc), group(rb)

    def last_sends(p):
        for w in qa:
            cols = parts(w)[p]
            for h in BOTH:
                wait(qa[w].at[h, 1:3, :, cols], rec2.at[w // 2, h, p, 1])

                def total2(t, w=w, h=h, cols=cols):
                    t = (*t, cols)
                    return total(w, h, 3, t) + qa[w][(h, 1, *t)].astype(F32) + qa[w][(h, 2, *t)].astype(F32)

                if w == UP:

                    def put2(t, total2=total2, cols=cols):
                        tall[UP][(*t, cols)] = total2(t)

                    tiles(w, put2)
                    cut(UP, h, cols)
                else:
                    n = fc.shape[1]
                    for b in BOTH:

                        def put2(i, total2=total2, h=h, b=b, n=n, cols=cols):
                            v = total2((pl.ds(pl.multiple_of(b * n + i * TILE, TILE), TILE),))
                            t = rows_of(i)
                            fc[2 * h + b, t, cols] = v
                            sc[2 * h + b, t, cols] = v.astype(BF)

                        fori(n // TILE, put2)
            if w == UP:
                for q in QUARTERS:
                    sa[q, :, cols] = pieces[UP][q, :, cols].astype(BF)
                fa[:, cols] = pieces[UP][z, :, cols]
            for j in FAR_FIRST:
                src, dst, left, axis = (sa, ra, left_a, "z") if w == UP else (sc, rc, left_c, "y")
                send(src.at[at(axis, j), :, cols], dst.at[j - 1, :, cols], left, rec3.at[w // 2, p], axis, j)

    def last_sends_down(k):
        for h in BOTH:
            wait(qb.at[h, k, 1:3], rec2b.at[h, k, 1])
            v = pb[h, k] + qb[h, k, 1].astype(F32) + qb[h, k, 2].astype(F32)
            off = offs(DOWN, h)[k]
            if off:
                bt[h, k] = v.astype(BF)
                send(bt.at[h, k], rb.at[h, k], left_b, rec3.at[2, h], "x", off)
            else:
                pb[h, k] = v

    first, second = BOTH
    running(first)
    running_down(0)
    running_down(1)
    running(second)
    running_down(2)
    running_down(3)
    last_sends(first)
    last_sends_down(0)
    last_sends_down(1)
    last_sends(second)
    last_sends_down(2)
    last_sends_down(3)

    def fold(v):
        v = jnp.sum(v * v, axis=0, keepdims=True)
        out = v[:, 0:128]
        for i in range(128, v.shape[1], 128):
            out = out + v[:, i : i + 128]
        nsend[...] = nsend[...] + out

    def rounded(own, others):
        for o in others:
            own = own + o.astype(F32)
        return own.astype(BF).astype(F32)

    others = range(len(FAR_FIRST))
    half = tsc.shape[-1]
    nsend[...] = jnp.zeros(nsend.shape, F32)
    for p in BOTH:
        wait(rc.at[:, :, parts(GATE)[p]], rec3.at[1, p])

    def last_c(i):
        t = rows_of(i)
        v = rounded(fc[y, t], [rc[j, t] for j in others])
        tall[UP][t, 0:half] = v
        fold(v)

    fori(fc.shape[1] // TILE, last_c)
    cut(GATE, 0)
    for q in QUARTERS:
        tsc[q] = pieces[GATE][q].astype(BF)
    tc[z] = tsc[z]
    left = group(tc.at[0:3])
    for j in FAR_FIRST:
        send(tsc.at[at("z", j)], tc.at[z], left, rech.at[0], "z", j)
    for p in BOTH:
        wait(ra.at[:, :, parts(UP)[p]], rec3.at[0, p])
    (gone,) = [i for i, (_, sem) in enumerate(leaving) if sem is left_a]
    wait(*leaving.pop(gone))
    v = rounded(fa[...], [ra[j] for j in others])
    gf[UP][...] = v
    fold(v)
    for h in BOTH:
        wait(rb.at[h], rec3.at[2, h])
        v = rounded(pb[h, 3], [rb[h, k] for k in others])
        gf[DOWN][:, down_cols(h)] = v
        fold(v)

    devices = nrecv.shape[0]
    nrecv[me] = nsend[...]
    left = group(nrecv.at[1:devices])
    away = [(min(i, N - i), i) for i in QUARTERS]
    for _, i, j, k in sorted((a + b + c, i, j, k) for a, i in away for b, j in away for c, k in away)[:0:-1]:
        post(nsend, nrecv.at[me], left, recn.at[0], to("x", i) + to("y", j) + to("z", k) - 2 * me)
    wait(tc.at[0:3], rech.at[0])
    wait(nrecv.at[1:devices], recn.at[0])
    squares = jnp.sum(jnp.sum(nrecv[...], axis=0), axis=1, keepdims=True)
    factor = jnp.minimum(1.0, 0.5 * lax.rsqrt(squares / count + 1e-30))
    rows = vi[GATE].shape[0]

    def gate_part(q):
        return slice(rows * (q // 2), rows * (q // 2 + 1)), slice(half * (q % 2), half * (q % 2 + 1))

    for q in QUARTERS:
        gf[GATE][gate_part(q)] = tc[q].astype(F32)[:rows]

    def adamw(w):
        gc = gf[w][...] * factor
        m = 0.9 * ms[w][...] + 0.1 * gc
        v = 0.95 * vs[w][...] + 0.05 * gc * gc
        mo[w][...] = m
        vo[w][...] = v
        step = m * lax.rsqrt(v + 1e-8) + 0.1 * ws[w][...]
        return ws[w][...] - 0.02 * step

    def spread_out(i, axis, ref, first):
        left = group(first)
        for j in FAR_FIRST:
            send(ref(co[axis]), ref(co[axis]), left, rech.at[i], axis, j)

    pieces[UP][0] = adamw(GATE)
    for q in QUARTERS:
        pieces[GATE][q, 0:rows] = pieces[UP][(0, *gate_part(q))]
        vc[q] = pieces[GATE][q].astype(BF)
    uc[z] = vc[z]
    left = group(uc.at[0:3])
    for j in FAR_FIRST:
        send(vc.at[at("z", j)], uc.at[z], left, rech.at[2], "z", j)
    ua[z] = adamw(UP).astype(BF)
    spread_out(1, "z", lambda p: ua.at[p], ua.at[0:3])
    ub[z, x] = adamw(DOWN).astype(BF)
    left = group(ub.at[0, 0:3])
    for j in FAR_FIRST:
        send(ub.at[z, x], ub.at[z, x], left, rech.at[N + j], "x", j)

    class Ring:
        def __init__(self, ref, sub, left, recv, axis):
            self.ref, self.sub, self.left, self.recv, self.axis = ref, sub, left, recv, axis

        def half(self, p, h):
            return self.ref(p).at[self.sub(h)]

        def own(self, h):
            for d in BOTH:
                ref = self.half(0, h)
                send(ref, ref, self.left, self.recv(d, h), self.axis, way(d))

        def owns(self):
            for h in BOTH:
                self.own(h)

        def pass_on(self):
            for d in BOTH:
                ref = self.half(NEAR[d], d)
                wait(ref, self.recv(d, d))
                send(ref, ref, self.left, self.recv(2, d), self.axis, way(d))

        def near(self, d):
            wait(self.half(NEAR[d], 1 - d), self.recv(d, 1 - d))

        def far(self):
            for d in BOTH:
                wait(self.half(2, d), self.recv(2, d))

    def one(h):
        return h

    def two(h):
        return pl.ds(2 * h, 2)

    def outer_ring(w, i, left):
        a, c = AXES[w][0], CHUNK_AXIS[w]
        return Ring(
            lambda p: W[w].at[at(a, p), at(c, OUTWARD[i])],
            two if w == GATE else one,
            left,
            lambda u, v: rec1.at[w, 0, u, i] if u == v else recd.at[w, u // 2],
            a,
        )

    left_o = [group(W[w].at[0:3]) for w in WEIGHTS]
    outer = [[outer_ring(w, i, left_o[w]) for i in QUARTERS] for w in WEIGHTS]
    left_z, left_y, left_x = group(ub.at[0:3]), group(W[UP].at[0, 0:3]), group(W[GATE].at[0, 0:3])
    zring = [
        Ring(lambda p, off=off: ub.at[at("z", p), at("x", off)], lambda h: (slice(None), down_cols(h)), left_z, lambda u, v, i=i: rec2b.at[u, i, 0] if u == v else rec2b.at[0, i, 1], "z")
        for i, off in enumerate(OUTWARD)
    ]
    yring = Ring(lambda p: W[UP].at[x, at("y", p)], one, left_y, lambda u, v: rec2.at[0, v, u % 2, u // 2], "y")
    xring = Ring(lambda p: W[GATE].at[z, at("x", p)], two, left_x, lambda u, v: rec2.at[1, v, u % 2, u // 2], "x")

    zring[0].owns()
    wait(uc.at[0:3], rech.at[2])
    for q in QUARTERS:
        pieces[GATE][q] = uc[q].astype(F32)
    W[GATE][z, x, y] = join(GATE, 0)
    spread_out(3, "y", lambda p: W[GATE].at[z, x, p], W[GATE].at[0, 0, 0:3])
    for i, off in enumerate(OUTWARD):
        if off:
            wait(ub.at[z, at("x", off)], rech.at[N - off % N + N])
            zring[i].owns()
    wait(ua.at[0:3], rech.at[1])
    for q in QUARTERS:
        pieces[UP][q] = ua[q].astype(F32)
    for h in BOTH:
        W[UP][x, y, h] = join(UP, h)
        yring.own(h)
        outer[UP][0].own(h)
    zring[0].pass_on()
    wait(W[GATE].at[0, 0, 0:3], rech.at[3])
    xring.owns()
    for i in QUARTERS:
        if i:
            zring[i].pass_on()
    outer[GATE][0].owns()
    yring.pass_on()
    for d in BOTH:
        yring.near(d)
    outer[UP][1].owns()
    for i in QUARTERS:
        wait(ub.at[0:2, 0], rec2b.at[0, i, 1])
        c = at("x", OUTWARD[i])
        for d in BOTH:
            for q in QUARTERS:
                pieces[DOWN][q] = ub[q, c, :, down_cols(d)].astype(F32)
            for h in BOTH:
                W[DOWN][y, c, h, :, down_cols(d)] = join(DOWN, h)
        outer[DOWN][i].owns()
    xring.pass_on()
    for d in BOTH:
        xring.near(d)
    outer[UP][2].owns()
    outer[GATE][1].owns()
    outer[GATE][2].owns()
    yring.far()
    outer[UP][3].owns()
    xring.far()
    outer[GATE][3].owns()
    for i in QUARTERS:
        for w in WEIGHTS:
            outer[w][i].pass_on()
    for w in WEIGHTS:
        for i in BOTH:
            wait(W[w].at[0], recd.at[w, i])
    for ref, sem in leaving:
        wait(ref, sem)


def write_kernel(names, *refs):
    R = dict(zip(names, refs, strict=True))
    W = [R["W", w] for w in WEIGHTS]
    out = [R["out", w] for w in WEIGHTS]
    half = W[GATE].shape[-1]
    copies = []
    for p in QUARTERS:
        for h in BOTH:
            cols, two = pl.ds(half * (p % 2), half), pl.ds(2 * h, 2)
            pairs = (
                (W[UP].at[p, :, h], out[UP].at[h, p]),
                (W[DOWN].at[p, :, h], out[DOWN].at[h, :, p]),
                (W[GATE].at[p, two], out[GATE].at[p // 2, two, :, :, cols]),
            )
            copies += [pltpu.make_async_copy(*pair, R["sem"].at[w, p, h]) for w, pair in enumerate(pairs)]
    for c in copies:
        c.start()
    for w in WEIGHTS:

        rows = R["mb", w].shape[0]

        def gather(i, w=w, rows=rows):
            for n in "mv":
                for h in BOTH:
                    R[n + "b", w][i, h : h + 1] = R[n + "o", w][pl.ds(rows * h + i, 1), :]

        fori(rows, gather)
        for i, n in enumerate("mv"):
            copies.append(pltpu.make_async_copy(R[n + "b", w], R[n + "out", w], R["small"].at[i, w]))
            copies[-1].start()
    for c in copies:
        c.wait()


def call(kernel, ins, outs, scratch, place_in, place_out, **params):
    names = (*ins, *outs, *scratch)
    got = pl.pallas_call(
        lambda *refs: kernel(names, *refs),
        out_shape=list(outs.values()),
        in_specs=[pl.BlockSpec(memory_space=place_in)] * len(ins),
        out_specs=[pl.BlockSpec(memory_space=place_out)] * len(outs),
        scratch_shapes=list(scratch.values()),
        name=kernel.__name__,
        compiler_params=pltpu.CompilerParams(**params),
    )(*ins.values())
    return dict(zip(outs, got, strict=True))


def by_weight(**of):
    return {(n, w): t for n, ts in of.items() for w, t in zip(WEIGHTS, ts)}


def solution(mesh):
    def step(*arrays):
        terms, weights, m, v = ([arrays[i + j] for j in (1, 2, 0)] for i in (0, 3, 6, 9))
        (rows, ff), (rows_d, d) = m[0].shape[1:], m[1].shape[1:]
        half, n, n_d = ff // 2, N * rows, N * rows_d
        full = ((2, N, N, n, ff), (2, N, N, n_d, d), (2, N, N, n, ff))
        g = [t.reshape(s) for t, s in zip(terms, (*full[:2], (2, N, 2, 2 * n, ff)))]
        state = [[pltpu.with_memory_space_constraint(a.transpose(1, 0, 2), pltpu.HBM) for a in t] for t in (m, v)]
        weights = [a.reshape(s) for a, s in zip(weights, full)]
        ins = by_weight(g=g, wt=weights, mi=state[0], vi=state[1])

        vm, dma = pltpu.VMEM, pltpu.SemaphoreType.DMA
        pad = TILE
        chunk = ((n, ff), (2, n_d, d // 2), (2 * n, half))
        own = ((2 * rows, ff), (2 * rows_d, d), (2 * rows, ff))
        down = (2 * rows_d, d // 2)
        pieces = [vm((N, *s), F32) for s in (own[0], down, (pad, half))]
        scratch = by_weight(
            own1=[vm((2, N, *c), BF) for c in chunk],
            own2=[vm((2, N, *c), BF) for c in chunk],
            early=[vm((2, *c), BF) for c in chunk],
            r=[vm((3, 2, N, *c), BF) for c in chunk],
            ws=[vm(s, F32) for s in own],
            ms=[vm(s, F32) for s in own],
            vs=[vm(s, F32) for s in own],
            pieces=pieces,
            wl=[vm((2, n, ff), BF), vm((2, n_d, d), BF)],
            mv=[vm((2, *a.shape), F32) for a in state[0][:2]],
            tall=[vm((n, ff), F32), vm((n_d, d // 2), F32)],
        )
        scratch |= {("qa", w): vm((2, 3, *chunk[w]), BF) for w in (UP, GATE)}
        scratch |= dict(
            pb=vm((2, N, *down), F32),
            bs=vm((2, N, 3, *down), BF),
            qb=vm((2, N, 3, *down), BF),
            bt=vm((2, 3, *down), BF),
            rb=vm((2, 3, *down), BF),
            fa=vm(own[0], F32),
            sa=vm((N, *own[0]), BF),
            ra=vm((3, *own[0]), BF),
            fc=vm((N, n, half), F32),
            sc=vm((N, n, half), BF),
            rc=vm((3, n, half), BF),
            tsc=vm((N, pad, half), BF),
            tc=vm((N, pad, half), BF),
            ub=vm((N, N, *own[1]), BF),
            uc=vm((N, pad, half), BF),
            vc=vm((N, pad, half), BF),
            nsend=vm((1, 128), F32),
            nrecv=vm((N**3, 1, 128), F32),
            sent=dma((24,)),
            local=dma((6, 3)),
            rec1=dma((3, 2, 2, N)),
            recd=dma((3, 2)),
            rec2=dma((2, 2, 2, 2)),
            rec2b=dma((2, N, 2)),
            rec3=dma((3, 2)),
            recn=dma((1,)),
            rech=dma((2 * N,)),
        )
        outs = by_weight(
            W=[jax.ShapeDtypeStruct(s, BF) for s in ((N, N, 2, n, ff), (N, N, 2, n_d, d), (N, N, N, n, half))],
            mo=[jax.ShapeDtypeStruct(s, F32) for s in own],
            vo=[jax.ShapeDtypeStruct(s, F32) for s in own],
        )
        count = float(N**3 * sum(a.size for a in m))

        def main(names, *refs):
            main_kernel(names, count, *refs)

        got = call(main, ins, outs, scratch, pltpu.HBM, vm, collective_id=0, has_side_effects=True, vmem_limit_bytes=37600000)
        small = [jax.ShapeDtypeStruct(a.shape, F32) for a in state[0]]
        outs = by_weight(out=[jax.ShapeDtypeStruct(s, BF) for s in full], mout=small, vout=small)
        scratch = by_weight(mb=[vm(a.shape, F32) for a in small], vb=[vm(a.shape, F32) for a in small])
        scratch |= dict(sem=dma((3, N, 2)), small=dma((2, 3)))
        new = call(write_kernel, got, outs, scratch, vm, pltpu.HBM, vmem_limit_bytes=2000000)
        back = (GATE, UP, DOWN)
        whole = [new["out", w].reshape(2, -1, full[w][-1]) for w in back]
        return (*whole, *(new[n, w].transpose(1, 0, 2) for n in ("mout", "vout") for w in back))

    all_of, part = P(None, None, None), P(None, "dp", None)
    return jax.shard_map(
        step,
        mesh=mesh,
        in_specs=(P(("rep", "dp"), None, None, None),) * 3 + (all_of,) * 3 + (part,) * 6,
        out_specs=(P("rep", None, None),) * 3 + (P("rep", "dp", None),) * 6,
        check_vma=False,
    )
```

```python
import jax
import jax.numpy as jnp
from jax import lax
from jax.experimental import pallas as pl
from jax.experimental.pallas import tpu as pltpu
from jax.sharding import PartitionSpec as P

UP, DOWN, GATE = WEIGHTS = range(3)
N = 4
QUARTERS = range(N)
FLOWS = BOTH = range(2)
ALL = [(w, h) for h in FLOWS for w in WEIGHTS]
STRIDE = {"x": N * N, "y": N, "z": 1}
AXES = (("x", "y", "z"), ("y", "z", "x"), ("z", "x", "y"))
CHUNK_AXIS = ("y", "x", "x")
FAR_FIRST = (2, 1, 3)
OUTWARD = (0, -1, 1, 2)
NEAR = (-1, 1)
TILE = 16
BF, F32 = jnp.bfloat16, jnp.float32


def fori(n, body):
    lax.fori_loop(0, n, lambda i, c: (body(i), c)[1], 0)


def main_kernel(names, count, *refs):
    R = dict(zip(names, refs, strict=True))

    def three(name):
        return [R[name, w] for w in WEIGHTS]

    g, wt, mi, vi, W, mo, vo = (three(n) for n in ("g", "wt", "mi", "vi", "W", "mo", "vo"))
    own1, own2, r, ws, ms, vs, pieces = (three(n) for n in ("own1", "own2", "r", "ws", "ms", "vs", "pieces"))
    wl, mv = ([R[n, UP], R[n, DOWN], R[n, UP]] for n in ("wl", "mv"))
    tall = [R["tall", UP], R["tall", DOWN], R["tall", UP]]
    qa = {w: R["qa", w] for w in (UP, GATE)}
    gf = mo
    pb, bs, qb, bt, rb, fa, sa, ra, fc, sc, rc, tsc, tc, ub, uc, vc, nsend, nrecv = (
        R[n] for n in ("pb", "bs", "qb", "bt", "rb", "fa", "sa", "ra", "fc", "sc", "rc", "tsc", "tc", "ub", "uc", "vc", "nsend", "nrecv")
    )
    ua = sa
    sent, local, rec1, recd, rec2, rec2b, rec3, recn, rech = (
        R[n] for n in ("sent", "local", "rec1", "recd", "rec2", "rec2b", "rec3", "recn", "rech")
    )
    tokens = iter(range(sent.shape[0]))
    leaving = []

    me = lax.axis_index("dp")
    co = {"x": me // STRIDE["x"], "y": me // STRIDE["y"] % N, "z": me % N}
    x, y, z = co["x"], co["y"], co["z"]

    def at(axis, off):
        return (co[axis] + off) % N

    def to(axis, off):
        return me + (at(axis, off) - co[axis]) * STRIDE[axis]

    def group(ref):
        sem = sent.at[next(tokens)]
        leaving.append((ref, sem))
        return sem

    def post(src, dst, ssem, rsem, device):
        pltpu.make_async_remote_copy(
            src_ref=src, dst_ref=dst, send_sem=ssem, recv_sem=rsem, device_id={"dp": device}, device_id_type=pl.DeviceIdType.MESH
        ).start()

    def send(src, dst, ssem, rsem, axis, off):
        post(src, dst, ssem, rsem, to(axis, off))

    def wait(ref, sem):
        pltpu.make_async_copy(ref, ref, sem).wait()

    def way(h):
        return 1 - 2 * h

    def offs(w, h):
        return (2, 1, -1, 0) if w == DOWN else (2, -way(h), way(h), 0)

    def term(w, h, q, c):
        if w == UP:
            return g[w].at[h, q, c]
        if w == DOWN:
            return g[w].at[:, c, q, :, down_cols(h)]
        cols = g[w].shape[-1] // 2
        return g[w].at[q // 2, c, h, :, pl.ds(pl.multiple_of(q % 2 * cols, 128), cols)]

    def rows_of(i):
        return pl.ds(pl.multiple_of(i * TILE, TILE), TILE)

    def tiles(w, body):
        n = own1[w].shape[-2] // TILE
        if w == DOWN:
            fori(2 * n, lambda i: body((i // n, rows_of(i % n))))
        else:
            fori(n, lambda i: body((rows_of(i),)))

    def parts(w):
        cols = own1[w].shape[-1]
        cut_at = (cols // 128 * 2 + 1) // 3 * 128
        return slice(0, cut_at), slice(cut_at, cols)

    def down_cols(h):
        cols = own1[DOWN].shape[-1]
        return pl.ds(h * cols, cols)

    def cut(w, h, part=slice(None)):
        rows, cols = vi[w].shape[0], pieces[w].shape[-1]
        for q in QUARTERS:
            pieces[w][q, rows * h : rows * (h + 1), part] = tall[w][rows * q : rows * (q + 1), 0:cols][:, part]

    def join(w, h):
        rows, cols = vi[w].shape[0], pieces[w].shape[-1]
        for q in QUARTERS:
            tall[w][rows * q : rows * (q + 1), 0:cols] = pieces[w][q, rows * h : rows * (h + 1)]
        return tall[w][0 : N * rows, 0:cols].astype(BF)

    barrier = pltpu.get_barrier_semaphore()
    for axis in STRIDE:
        for off in NEAR:
            pl.semaphore_signal(barrier, inc=1, device_id={"dp": to(axis, off)}, device_id_type=pl.DeviceIdType.MESH)

    early = three("early")

    def first_term(w, h):
        return term(w, h, at(AXES[w][0], 2), at(CHUNK_AXIS[w], offs(w, h)[0]))

    for w, h in ALL:
        pltpu.make_async_copy(first_term(w, h), early[w].at[h], local.at[N, w]).start()
    for which, buf in enumerate((own1, own2)):
        for w, h in ALL:
            q = at(AXES[w][0], way(h) * (1 - which))
            for k in QUARTERS:
                src = term(w, h, q, at(CHUNK_AXIS[w], offs(w, h)[k]))
                pltpu.make_async_copy(src, buf[w].at[h, k], local.at[which, w]).start()
    pl.semaphore_wait(barrier, len(STRIDE) * len(NEAR))

    for w in WEIGHTS:
        wait(early[w], local.at[N, w])
    left1 = [group(r[w]) for w in WEIGHTS]

    def phase1(i, w, h, k, src, off):
        sem = recd.at[w, h] if i == 1 else rec1.at[w, i // 2, h, k]
        send(src, r[w].at[i, h, k], left1[w], sem, AXES[w][0], off)

    for i, (far, near) in enumerate(((2, 1), (-1, -1))):
        for k in QUARTERS:
            for w, h in ALL:
                s = way(h)
                src = early[w].at[h]
                if i or k:
                    src = term(w, h, at(AXES[w][0], far * s), at(CHUNK_AXIS[w], offs(w, h)[k]))
                phase1(i, w, h, k, src, near * s)

    def load_state(w):
        for i, (src, dst) in enumerate(((wt[w].at[:, x, y], wl[w]), (mi[w], mv[w].at[0]), (vi[w], mv[w].at[1]))):
            pltpu.make_async_copy(src, dst, local.at[2 + min(i, 1), w]).start()

    load_state(UP)
    load_state(DOWN)
    for which, buf in enumerate((own1, own2)):
        for w in WEIGHTS:
            wait(buf[w], local.at[which, w])

    for k in QUARTERS:
        for w, h in ALL:
            wait(r[w].at[0, h, k], rec1.at[w, 0, h, k])

            def add(t, w=w, h=h, k=k):
                t = (h, k, *t)
                own1[w][t] = (own1[w][t].astype(F32) + r[w][(0, *t)].astype(F32)).astype(BF)

            tiles(w, add)
            phase1(2, w, h, k, own1[w].at[h, k], way(h))

    pieces[GATE][...] = jnp.zeros(pieces[GATE].shape, F32)
    for w in WEIGHTS:
        rows = vi[w].shape[0]
        for i, dst in enumerate((wl[w], mv[w])):
            wait(dst, local.at[2 + i, w])

        def spread(i, w=w, rows=rows):
            for src, dst in ((mv[w][0, i], ms[w]), (mv[w][1, i], vs[w])):
                for h in BOTH:
                    dst[pl.ds(rows * h + i, 1), :] = src[h : h + 1]

        fori(rows, spread)
        v = DOWN if w == DOWN else UP
        for cols in [down_cols(c) for c in BOTH] if w == DOWN else [slice(None)]:
            for h in BOTH:

                def widen(i, w=w, h=h, v=v, cols=cols):
                    t = rows_of(i)
                    tall[v][t, :] = wl[w][h, t, cols].astype(F32)

                fori(N * rows // TILE, widen)
                cut(v, h)
            ws[w][:, cols] = pieces[v][z]
        if w == UP:
            load_state(GATE)

    def total(w, h, k, t):
        t = (h, k, *t)
        return own2[w][t].astype(F32) + r[w][(1, *t)].astype(F32) + r[w][(2, *t)].astype(F32)

    def cut_down(h, k):
        n = own2[DOWN].shape[-2]
        for layer in BOTH:

            def put(i, layer=layer):
                t = rows_of(i)
                tall[DOWN][t, :] = total(DOWN, h, k, (layer, t))

            fori(n // TILE, put)
            cut(DOWN, layer)

    left2 = {w: group(qa[w]) for w in qa}
    left2b = group(qb)

    def phase2(i, w, h, off, part=None):
        for p in BOTH if part is None else (part,):
            cols = (slice(None), parts(w)[p])
            src, dst = own2[w].at[h, i], qa[w].at[h, i]
            send(src.at[cols], dst.at[cols], left2[w], rec2.at[w // 2, h, p, min(i, 1)], AXES[w][1], off)

    def phase2b(i, h, k, off):
        send(bs.at[h, k, i], qb.at[h, k, i], left2b, rec2b.at[h, k, min(i, 1)], "z", off)

    for k in QUARTERS:
        for w, h in ALL:
            s = way(h)
            if not k:
                wait(r[w].at[1, h], recd.at[w, h])
            wait(r[w].at[2, h, k], rec1.at[w, 1, h, k])
            if w == DOWN:
                cut_down(h, k)
                pb[h, k] = pieces[w][z]
                for i, (far, near) in enumerate(((2, 1), (-1, -1))):
                    bs[h, k, i] = pieces[w][at("z", far * s)].astype(BF)
                    phase2b(i, h, k, near * s)
            elif k < 2:

                def put(t, w=w, h=h, k=k):
                    own2[w][(h, k, *t)] = total(w, h, k, t).astype(BF)

                tiles(w, put)
                phase2(k, w, h, -s if k else s)

    def running(p):
        for w in qa:
            cols = parts(w)[p]
            for h in FLOWS:
                wait(qa[w].at[h, 0, :, cols], rec2.at[w // 2, h, p, 0])

                def add2(t, w=w, h=h, cols=cols):
                    t = (*t, cols)
                    own2[w][(h, 2, *t)] = (total(w, h, 2, t) + qa[w][(h, 0, *t)].astype(F32)).astype(BF)

                tiles(w, add2)
                phase2(2, w, h, way(h), p)

    def running_down(k):
        for h in FLOWS:
            s = way(h)
            cut_down(h, k)
            wait(qb.at[h, k, 0], rec2b.at[h, k, 0])
            bs[h, k, 2] = (pieces[DOWN][at("z", s)] + qb[h, k, 0].astype(F32)).astype(BF)
            phase2b(2, h, k, s)

    left_a, left_c, left_b = group(ra), group(rc), group(rb)

    def last_sends(p):
        for w in qa:
            cols = parts(w)[p]
            for h in BOTH:
                wait(qa[w].at[h, 1:3, :, cols], rec2.at[w // 2, h, p, 1])

                def total2(t, w=w, h=h, cols=cols):
                    t = (*t, cols)
                    return total(w, h, 3, t) + qa[w][(h, 1, *t)].astype(F32) + qa[w][(h, 2, *t)].astype(F32)

                if w == UP:

                    def put2(t, total2=total2, cols=cols):
                        tall[UP][(*t, cols)] = total2(t)

                    tiles(w, put2)
                    cut(UP, h, cols)
                else:
                    n = fc.shape[1]
                    for b in BOTH:

                        def put2(i, total2=total2, h=h, b=b, n=n, cols=cols):
                            v = total2((pl.ds(pl.multiple_of(b * n + i * TILE, TILE), TILE),))
                            t = rows_of(i)
                            fc[2 * h + b, t, cols] = v
                            sc[2 * h + b, t, cols] = v.astype(BF)

                        fori(n // TILE, put2)
            if w == UP:
                for q in QUARTERS:
                    sa[q, :, cols] = pieces[UP][q, :, cols].astype(BF)
                fa[:, cols] = pieces[UP][z, :, cols]
            for j in FAR_FIRST:
                src, dst, left, axis = (sa, ra, left_a, "z") if w == UP else (sc, rc, left_c, "y")
                send(src.at[at(axis, j), :, cols], dst.at[j - 1, :, cols], left, rec3.at[w // 2, p], axis, j)

    def last_sends_down(k):
        for h in BOTH:
            wait(qb.at[h, k, 1:3], rec2b.at[h, k, 1])
            v = pb[h, k] + qb[h, k, 1].astype(F32) + qb[h, k, 2].astype(F32)
            off = offs(DOWN, h)[k]
            if off:
                bt[h, k] = v.astype(BF)
                send(bt.at[h, k], rb.at[h, k], left_b, rec3.at[2, h], "x", off)
            else:
                pb[h, k] = v

    first, second = BOTH
    running(first)
    running_down(0)
    running_down(1)
    running(second)
    running_down(2)
    running_down(3)
    last_sends(first)
    last_sends_down(0)
    last_sends_down(1)
    last_sends(second)
    last_sends_down(2)
    last_sends_down(3)

    def fold(v):
        v = jnp.sum(v * v, axis=0, keepdims=True)
        out = v[:, 0:128]
        for i in range(128, v.shape[1], 128):
            out = out + v[:, i : i + 128]
        nsend[...] = nsend[...] + out

    def rounded(own, others):
        for o in others:
            own = own + o.astype(F32)
        return own.astype(BF).astype(F32)

    others = range(len(FAR_FIRST))
    half = tsc.shape[-1]
    nsend[...] = jnp.zeros(nsend.shape, F32)
    for p in BOTH:
        wait(rc.at[:, :, parts(GATE)[p]], rec3.at[1, p])

    def last_c(i):
        t = rows_of(i)
        v = rounded(fc[y, t], [rc[j, t] for j in others])
        tall[UP][t, 0:half] = v
        fold(v)

    fori(fc.shape[1] // TILE, last_c)
    cut(GATE, 0)
    for q in QUARTERS:
        tsc[q] = pieces[GATE][q].astype(BF)
    tc[z] = tsc[z]
    left = group(tc.at[0:3])
    for j in FAR_FIRST:
        send(tsc.at[at("z", j)], tc.at[z], left, rech.at[0], "z", j)
    for p in BOTH:
        wait(ra.at[:, :, parts(UP)[p]], rec3.at[0, p])
    (gone,) = [i for i, (_, sem) in enumerate(leaving) if sem is left_a]
    wait(*leaving.pop(gone))
    v = rounded(fa[...], [ra[j] for j in others])
    gf[UP][...] = v
    fold(v)
    for h in BOTH:
        wait(rb.at[h], rec3.at[2, h])
        v = rounded(pb[h, 3], [rb[h, k] for k in others])
        gf[DOWN][:, down_cols(h)] = v
        fold(v)

    devices = nrecv.shape[0]
    nrecv[me] = nsend[...]
    left = group(nrecv.at[1:devices])
    away = [(min(i, N - i), i) for i in QUARTERS]
    for _, i, j, k in sorted((a + b + c, i, j, k) for a, i in away for b, j in away for c, k in away)[:0:-1]:
        post(nsend, nrecv.at[me], left, recn.at[0], to("x", i) + to("y", j) + to("z", k) - 2 * me)
    wait(tc.at[0:3], rech.at[0])
    wait(nrecv.at[1:devices], recn.at[0])
    squares = jnp.sum(jnp.sum(nrecv[...], axis=0), axis=1, keepdims=True)
    factor = jnp.minimum(1.0, 0.5 * lax.rsqrt(squares / count + 1e-30))
    rows = vi[GATE].shape[0]

    def gate_part(q):
        return slice(rows * (q // 2), rows * (q // 2 + 1)), slice(half * (q % 2), half * (q % 2 + 1))

    for q in QUARTERS:
        gf[GATE][gate_part(q)] = tc[q].astype(F32)[:rows]

    def adamw(w):
        gc = gf[w][...] * factor
        m = 0.9 * ms[w][...] + 0.1 * gc
        v = 0.95 * vs[w][...] + 0.05 * gc * gc
        mo[w][...] = m
        vo[w][...] = v
        step = m * lax.rsqrt(v + 1e-8) + 0.1 * ws[w][...]
        return ws[w][...] - 0.02 * step

    def spread_out(i, axis, ref, first):
        left = group(first)
        for j in FAR_FIRST:
            send(ref(co[axis]), ref(co[axis]), left, rech.at[i], axis, j)

    pieces[UP][0] = adamw(GATE)
    for q in QUARTERS:
        pieces[GATE][q, 0:rows] = pieces[UP][(0, *gate_part(q))]
        vc[q] = pieces[GATE][q].astype(BF)
    uc[z] = vc[z]
    left = group(uc.at[0:3])
    for j in FAR_FIRST:
        send(vc.at[at("z", j)], uc.at[z], left, rech.at[2], "z", j)
    ua[z] = adamw(UP).astype(BF)
    spread_out(1, "z", lambda p: ua.at[p], ua.at[0:3])
    ub[z, x] = adamw(DOWN).astype(BF)
    left = group(ub.at[0, 0:3])
    for j in FAR_FIRST:
        send(ub.at[z, x], ub.at[z, x], left, rech.at[N + j], "x", j)

    class Ring:
        def __init__(self, ref, sub, left, recv, axis):
            self.ref, self.sub, self.left, self.recv, self.axis = ref, sub, left, recv, axis

        def half(self, p, h):
            return self.ref(p).at[self.sub(h)]

        def own(self, h):
            for d in BOTH:
                ref = self.half(0, h)
                send(ref, ref, self.left, self.recv(d, h), self.axis, way(d))

        def owns(self):
            for h in BOTH:
                self.own(h)

        def pass_on(self):
            for d in BOTH:
                ref = self.half(NEAR[d], d)
                wait(ref, self.recv(d, d))
                send(ref, ref, self.left, self.recv(2, d), self.axis, way(d))

        def near(self, d):
            wait(self.half(NEAR[d], 1 - d), self.recv(d, 1 - d))

        def far(self):
            for d in BOTH:
                wait(self.half(2, d), self.recv(2, d))

    def one(h):
        return h

    def two(h):
        return pl.ds(2 * h, 2)

    def outer_ring(w, i, left):
        a, c = AXES[w][0], CHUNK_AXIS[w]
        return Ring(
            lambda p: W[w].at[at(a, p), at(c, OUTWARD[i])],
            two if w == GATE else one,
            left,
            lambda u, v: rec1.at[w, 0, u, i] if u == v else recd.at[w, u // 2],
            a,
        )

    left_o = [group(W[w].at[0:3]) for w in WEIGHTS]
    outer = [[outer_ring(w, i, left_o[w]) for i in QUARTERS] for w in WEIGHTS]
    left_z, left_y, left_x = group(ub.at[0:3]), group(W[UP].at[0, 0:3]), group(W[GATE].at[0, 0:3])
    zring = [
        Ring(lambda p, off=off: ub.at[at("z", p), at("x", off)], lambda h: (slice(None), down_cols(h)), left_z, lambda u, v, i=i: rec2b.at[u, i, 0] if u == v else rec2b.at[0, i, 1], "z")
        for i, off in enumerate(OUTWARD)
    ]
    yring = Ring(lambda p: W[UP].at[x, at("y", p)], one, left_y, lambda u, v: rec2.at[0, v, u % 2, u // 2], "y")
    xring = Ring(lambda p: W[GATE].at[z, at("x", p)], two, left_x, lambda u, v: rec2.at[1, v, u % 2, u // 2], "x")

    zring[0].owns()
    wait(uc.at[0:3], rech.at[2])
    for q in QUARTERS:
        pieces[GATE][q] = uc[q].astype(F32)
    W[GATE][z, x, y] = join(GATE, 0)
    spread_out(3, "y", lambda p: W[GATE].at[z, x, p], W[GATE].at[0, 0, 0:3])
    for i, off in enumerate(OUTWARD):
        if off:
            wait(ub.at[z, at("x", off)], rech.at[N - off % N + N])
            zring[i].owns()
    wait(ua.at[0:3], rech.at[1])
    for q in QUARTERS:
        pieces[UP][q] = ua[q].astype(F32)
    for h in BOTH:
        W[UP][x, y, h] = join(UP, h)
        yring.own(h)
        outer[UP][0].own(h)
    zring[0].pass_on()
    wait(W[GATE].at[0, 0, 0:3], rech.at[3])
    xring.owns()
    for i in QUARTERS:
        if i:
            zring[i].pass_on()
    outer[GATE][0].owns()
    yring.pass_on()
    for d in BOTH:
        yring.near(d)
    outer[UP][1].owns()
    for i in QUARTERS:
        wait(ub.at[0:2, 0], rec2b.at[0, i, 1])
        c = at("x", OUTWARD[i])
        for d in BOTH:
            for q in QUARTERS:
                pieces[DOWN][q] = ub[q, c, :, down_cols(d)].astype(F32)
            for h in BOTH:
                W[DOWN][y, c, h, :, down_cols(d)] = join(DOWN, h)
        outer[DOWN][i].owns()
    xring.pass_on()
    for d in BOTH:
        xring.near(d)
    outer[UP][2].owns()
    outer[GATE][1].owns()
    outer[GATE][2].owns()
    yring.far()
    outer[UP][3].owns()
    xring.far()
    outer[GATE][3].owns()
    for i in QUARTERS:
        for w in WEIGHTS:
            outer[w][i].pass_on()
    for w in WEIGHTS:
        for i in BOTH:
            wait(W[w].at[0], recd.at[w, i])
    for ref, sem in leaving:
        wait(ref, sem)


def write_kernel(names, *refs):
    R = dict(zip(names, refs, strict=True))
    W = [R["W", w] for w in WEIGHTS]
    out = [R["out", w] for w in WEIGHTS]
    half = W[GATE].shape[-1]
    copies = []
    for p in QUARTERS:
        for h in BOTH:
            cols, two = pl.ds(half * (p % 2), half), pl.ds(2 * h, 2)
            pairs = (
                (W[UP].at[p, :, h], out[UP].at[h, p]),
                (W[DOWN].at[p, :, h], out[DOWN].at[h, :, p]),
                (W[GATE].at[p, two], out[GATE].at[p // 2, two, :, :, cols]),
            )
            copies += [pltpu.make_async_copy(*pair, R["sem"].at[w, p, h]) for w, pair in enumerate(pairs)]
    for c in copies:
        c.start()
    for w in WEIGHTS:

        rows = R["mb", w].shape[0]

        def gather(i, w=w, rows=rows):
            for n in "mv":
                for h in BOTH:
                    R[n + "b", w][i, h : h + 1] = R[n + "o", w][pl.ds(rows * h + i, 1), :]

        fori(rows, gather)
        for i, n in enumerate("mv"):
            copies.append(pltpu.make_async_copy(R[n + "b", w], R[n + "out", w], R["small"].at[i, w]))
            copies[-1].start()
    for c in copies:
        c.wait()


def call(kernel, ins, outs, scratch, place_in, place_out, **params):
    names = (*ins, *outs, *scratch)
    got = pl.pallas_call(
        lambda *refs: kernel(names, *refs),
        out_shape=list(outs.values()),
        in_specs=[pl.BlockSpec(memory_space=place_in)] * len(ins),
        out_specs=[pl.BlockSpec(memory_space=place_out)] * len(outs),
        scratch_shapes=list(scratch.values()),
        name=kernel.__name__,
        compiler_params=pltpu.CompilerParams(**params),
    )(*ins.values())
    return dict(zip(outs, got, strict=True))


def by_weight(**of):
    return {(n, w): t for n, ts in of.items() for w, t in zip(WEIGHTS, ts)}


def solution(mesh):
    def step(*arrays):
        terms, weights, m, v = ([arrays[i + j] for j in (1, 2, 0)] for i in (0, 3, 6, 9))
        (rows, ff), (rows_d, d) = m[0].shape[1:], m[1].shape[1:]
        half, n, n_d = ff // 2, N * rows, N * rows_d
        full = ((2, N, N, n, ff), (2, N, N, n_d, d), (2, N, N, n, ff))
        g = [t.reshape(s) for t, s in zip(terms, (*full[:2], (2, N, 2, 2 * n, ff)))]
        state = [[pltpu.with_memory_space_constraint(a.transpose(1, 0, 2), pltpu.HBM) for a in t] for t in (m, v)]
        weights = [a.reshape(s) for a, s in zip(weights, full)]
        ins = by_weight(g=g, wt=weights, mi=state[0], vi=state[1])

        vm, dma = pltpu.VMEM, pltpu.SemaphoreType.DMA
        pad = TILE
        chunk = ((n, ff), (2, n_d, d // 2), (2 * n, half))
        own = ((2 * rows, ff), (2 * rows_d, d), (2 * rows, ff))
        down = (2 * rows_d, d // 2)
        pieces = [vm((N, *s), F32) for s in (own[0], down, (pad, half))]
        scratch = by_weight(
            own1=[vm((2, N, *c), BF) for c in chunk],
            own2=[vm((2, N, *c), BF) for c in chunk],
            early=[vm((2, *c), BF) for c in chunk],
            r=[vm((3, 2, N, *c), BF) for c in chunk],
            ws=[vm(s, F32) for s in own],
            ms=[vm(s, F32) for s in own],
            vs=[vm(s, F32) for s in own],
            pieces=pieces,
            wl=[vm((2, n, ff), BF), vm((2, n_d, d), BF)],
            mv=[vm((2, *a.shape), F32) for a in state[0][:2]],
            tall=[vm((n, ff), F32), vm((n_d, d // 2), F32)],
        )
        scratch |= {("qa", w): vm((2, 3, *chunk[w]), BF) for w in (UP, GATE)}
        scratch |= dict(
            pb=vm((2, N, *down), F32),
            bs=vm((2, N, 3, *down), BF),
            qb=vm((2, N, 3, *down), BF),
            bt=vm((2, 3, *down), BF),
            rb=vm((2, 3, *down), BF),
            fa=vm(own[0], F32),
            sa=vm((N, *own[0]), BF),
            ra=vm((3, *own[0]), BF),
            fc=vm((N, n, half), F32),
            sc=vm((N, n, half), BF),
            rc=vm((3, n, half), BF),
            tsc=vm((N, pad, half), BF),
            tc=vm((N, pad, half), BF),
            ub=vm((N, N, *own[1]), BF),
            uc=vm((N, pad, half), BF),
            vc=vm((N, pad, half), BF),
            nsend=vm((1, 128), F32),
            nrecv=vm((N**3, 1, 128), F32),
            sent=dma((21,)),
            local=dma((N + 1, 3)),
            rec1=dma((3, 2, 2, N)),
            recd=dma((3, 2)),
            rec2=dma((2, 2, 2, 2)),
            rec2b=dma((2, N, 2)),
            rec3=dma((3, 2)),
            recn=dma((1,)),
            rech=dma((2 * N,)),
        )
        outs = by_weight(
            W=[jax.ShapeDtypeStruct(s, BF) for s in ((N, N, 2, n, ff), (N, N, 2, n_d, d), (N, N, N, n, half))],
            mo=[jax.ShapeDtypeStruct(s, F32) for s in own],
            vo=[jax.ShapeDtypeStruct(s, F32) for s in own],
        )
        count = float(N**3 * sum(a.size for a in m))

        def main(names, *refs):
            main_kernel(names, count, *refs)

        got = call(main, ins, outs, scratch, pltpu.HBM, vm, collective_id=0, has_side_effects=True, vmem_limit_bytes=37600000)
        small = [jax.ShapeDtypeStruct(a.shape, F32) for a in state[0]]
        outs = by_weight(out=[jax.ShapeDtypeStruct(s, BF) for s in full], mout=small, vout=small)
        scratch = by_weight(mb=[vm(a.shape, F32) for a in small], vb=[vm(a.shape, F32) for a in small])
        scratch |= dict(sem=dma((3, N, 2)), small=dma((2, 3)))
        new = call(write_kernel, got, outs, scratch, vm, pltpu.HBM, vmem_limit_bytes=2000000)
        back = (GATE, UP, DOWN)
        whole = [new["out", w].reshape(2, -1, full[w][-1]) for w in back]
        return (*whole, *(new[n, w].transpose(1, 0, 2) for n in ("mout", "vout") for w in back))

    all_of, part = P(None, None, None), P(None, "dp", None)
    return jax.shard_map(
        step,
        mesh=mesh,
        in_specs=(P(("rep", "dp"), None, None, None),) * 3 + (all_of,) * 3 + (part,) * 6,
        out_specs=(P("rep", None, None),) * 3 + (P("rep", "dp", None),) * 6,
        check_vma=False,
    )
```
